32 devices in a mesh: dp: 32 (over z, y, x, core).
Axes of the slice: x: 2, y: 2, z: 4, core: 2. Of those that a mesh axis runs over, the one named last changes fastest.
Arguments:
- tokens: bfloat16 [32768, 768], P('dp')
- w_one: bfloat16 [768, 3072], replicated
- w_two: bfloat16 [3072, 768], replicated
- wi_one: bfloat16 [768, 3072], replicated
- wi_two: bfloat16 [3072, 768], replicated
- item_table: bfloat16 [131072, 768], P('dp')
- cand_ids: int32 [2048], replicated
- log_q: float32 [2048], replicated
- targets: int32 [32768], P('dp')
Outputs:
- output 1: float32 [], replicated
- output 2: float32 [131072, 768], P('dp')
- output 3: float32 [768, 3072], replicated
- output 4: float32 [3072, 768], replicated
- output 5: float32 [768, 3072], replicated
- output 6: float32 [3072, 768], replicated
All inputs are finite; a program needn't handle non-finite values.
Results may differ from the reference program's by a relative error of at most 0.00949047.
Values are sent between devices in bfloat16 or wider.
A program may use at most 1 GiB of HBM per device.

```python
import math
import jax
import jax.numpy as jnp
from jax import lax

DIN = 768
FF = 3072
D = 768
FF2 = 3072
TOK_DEV = 1024
CANDS = 2048
ROWS_DEV = 4096
DEVS = 32

TOKENS = TOK_DEV * DEVS
ROWS = ROWS_DEV * DEVS
HEAD_ROWS = 4 * CANDS
SCORE_GAIN = 3.0
HIT_VALUE = -1e9


def setup_inputs(seed: int = 0) -> dict:
    root_key = jax.random.key(seed)
    val_keys = jax.random.split(root_key, 7)
    tokens = jax.random.normal(val_keys[0], (TOKENS, DIN), jnp.float32).astype(jnp.bfloat16)
    w_one = (jax.random.normal(val_keys[1], (DIN, FF), jnp.float32) * DIN ** -0.5).astype(jnp.bfloat16)
    w_two = (jax.random.normal(val_keys[2], (FF, D), jnp.float32) * FF ** -0.5).astype(jnp.bfloat16)
    wi_one = (jax.random.normal(val_keys[3], (D, FF2), jnp.float32) * D ** -0.5).astype(jnp.bfloat16)
    wi_two = (jax.random.normal(val_keys[4], (FF2, D), jnp.float32) * FF2 ** -0.5).astype(jnp.bfloat16)
    item_table = jax.random.normal(val_keys[5], (ROWS, D), jnp.float32).astype(jnp.bfloat16)
    log_q = math.log(CANDS) + jax.random.uniform(val_keys[6], (CANDS,), jnp.float32, -3.0, 3.0)
    int_keys = jax.random.split(jax.random.fold_in(root_key, 1), 7)
    head_ids = jax.random.permutation(int_keys[0], HEAD_ROWS)[: CANDS // 2]
    tail_ids = HEAD_ROWS + jax.random.permutation(int_keys[1], ROWS - HEAD_ROWS)[: CANDS - CANDS // 2]
    cand_ids = jnp.concatenate([head_ids, tail_ids])[jax.random.permutation(int_keys[2], CANDS)].astype(jnp.int32)
    pick_mode = jax.random.randint(int_keys[3], (TOKENS,), 0, 4)
    from_cands = cand_ids[jax.random.randint(int_keys[4], (TOKENS,), 0, CANDS)]
    from_head = jax.random.randint(int_keys[5], (TOKENS,), 0, HEAD_ROWS)
    from_all = jax.random.randint(int_keys[6], (TOKENS,), 0, ROWS)
    targets = jnp.where(pick_mode == 0, from_cands, jnp.where(pick_mode == 1, from_head, from_all)).astype(jnp.int32)
    return {"tokens": tokens, "w_one": w_one, "w_two": w_two, "wi_one": wi_one, "wi_two": wi_two, "item_table": item_table, "cand_ids": cand_ids, "log_q": log_q, "targets": targets}


def tower_fwd(row_block, w_in, w_out):
    pre_act = jnp.dot(row_block, w_in, preferred_element_type=jnp.float32)
    hidden = jax.nn.gelu(pre_act).astype(jnp.bfloat16)
    tower_out = jnp.dot(hidden, w_out, preferred_element_type=jnp.float32).astype(jnp.bfloat16)
    return pre_act, hidden, tower_out


def tower_back(row_block, w_out, pre_act, hidden, grad_out):
    dw_out = jnp.dot(hidden.T, grad_out, preferred_element_type=jnp.float32)
    grad_hidden = jnp.dot(grad_out, w_out.T, preferred_element_type=jnp.float32)
    gelu_back = jax.vjp(jax.nn.gelu, pre_act)[1]
    grad_pre = gelu_back(grad_hidden)[0].astype(jnp.bfloat16)
    dw_in = jnp.dot(row_block.T, grad_pre, preferred_element_type=jnp.float32)
    return grad_pre, dw_in, dw_out


def reference(tokens, w_one, w_two, wi_one, wi_two, item_table, cand_ids, log_q, targets):
    logit_scale = SCORE_GAIN / math.sqrt(D)
    cand_raw = item_table[cand_ids]
    c_pre, c_hidden, cand_vec = tower_fwd(cand_raw, wi_one, wi_two)

    def block_step(carry, blk):
        loss_acc, dcand_acc, dw_one_acc, dw_two_acc, dwi_one_acc, dwi_two_acc = carry
        tok_blk, targ_blk = blk
        q_pre, q_hidden, query = tower_fwd(tok_blk, w_one, w_two)
        targ_raw = item_table[targ_blk]
        t_pre, t_hidden, targ_vec = tower_fwd(targ_raw, wi_one, wi_two)
        z_targ = jnp.sum(query.astype(jnp.float32) * targ_vec.astype(jnp.float32), axis=1) * logit_scale
        z_cand = jnp.dot(query, cand_vec.T, preferred_element_type=jnp.float32) * logit_scale - log_q[None, :]
        z_cand = jnp.where(targ_blk[:, None] == cand_ids[None, :], HIT_VALUE, z_cand)
        row_max = jnp.maximum(z_targ, jnp.max(z_cand, axis=1))
        e_targ = jnp.exp(z_targ - row_max)
        e_cand = jnp.exp(z_cand - row_max[:, None])
        denom_sum = e_targ + jnp.sum(e_cand, axis=1)
        loss_blk = jnp.sum(jnp.log(denom_sum) + row_max - z_targ)
        dz_targ = ((e_targ / denom_sum - 1.0) / TOKENS).astype(jnp.bfloat16).astype(jnp.float32)
        dz_cand = (e_cand / denom_sum[:, None] / TOKENS).astype(jnp.bfloat16)
        d_query = ((dz_targ[:, None] * targ_vec.astype(jnp.float32) + jnp.dot(dz_cand, cand_vec, preferred_element_type=jnp.float32)) * logit_scale).astype(jnp.bfloat16)
        d_targ_vec = (logit_scale * dz_targ[:, None] * query.astype(jnp.float32)).astype(jnp.bfloat16)
        dcand_new = dcand_acc + jnp.dot(dz_cand.T, query, preferred_element_type=jnp.float32)
        dw_one_blk, dw_two_blk = tower_back(tok_blk, w_two, q_pre, q_hidden, d_query)[1:]
        t_grad_pre, dwi_one_blk, dwi_two_blk = tower_back(targ_raw, wi_two, t_pre, t_hidden, d_targ_vec)
        d_targ_raw = jnp.dot(t_grad_pre, wi_one.T, preferred_element_type=jnp.float32).astype(jnp.bfloat16)
        new_carry = (loss_acc + loss_blk, dcand_new, dw_one_acc + dw_one_blk, dw_two_acc + dw_two_blk, dwi_one_acc + dwi_one_blk, dwi_two_acc + dwi_two_blk)
        return new_carry, d_targ_raw

    init_carry = (jnp.zeros((), jnp.float32), jnp.zeros((CANDS, D), jnp.float32), jnp.zeros((DIN, FF), jnp.float32), jnp.zeros((FF, D), jnp.float32), jnp.zeros((D, FF2), jnp.float32), jnp.zeros((FF2, D), jnp.float32))
    tok_blocks = tokens.reshape(DEVS, TOK_DEV, DIN)
    targ_blocks = targets.reshape(DEVS, TOK_DEV)
    final_carry, d_targ_rows = lax.scan(block_step, init_carry, (tok_blocks, targ_blocks))
    loss_acc, dcand_acc, dw_one, dw_two, dwi_one_t, dwi_two_t = final_carry
    d_cand_vec = (logit_scale * dcand_acc).astype(jnp.bfloat16)
    c_grad_pre, dwi_one_c, dwi_two_c = tower_back(cand_raw, wi_two, c_pre, c_hidden, d_cand_vec)
    d_cand_raw = jnp.dot(c_grad_pre, wi_one.T, preferred_element_type=jnp.float32).astype(jnp.bfloat16)
    row_grads = jnp.concatenate([d_cand_raw, d_targ_rows.reshape(TOKENS, D)]).astype(jnp.float32)
    row_ids = jnp.concatenate([cand_ids, targets])
    d_table = jax.ops.segment_sum(row_grads, row_ids, num_segments=ROWS)
    return loss_acc / TOKENS, d_table, dw_one, dw_two, dwi_one_t + dwi_one_c, dwi_two_t + dwi_two_c
```

```python
import functools
import math
import jax
import jax.numpy as jnp
from jax import lax
from jax.experimental import pallas as pl
from jax.experimental.pallas import tpu as pltpu
from jax.sharding import PartitionSpec as P

SCORE_GAIN = 3.0
HIT_VALUE = -1e9
PAIR_ROWS = 48
HOT_ROWS = 240
MESH = pl.DeviceIdType.MESH
ANY = pl.BlockSpec(memory_space=pl.ANY)


def tower_fwd(row_block, w_in, w_out):
    pre_act = jnp.dot(row_block, w_in, preferred_element_type=jnp.float32)
    hidden = jax.nn.gelu(pre_act).astype(jnp.bfloat16)
    tower_out = jnp.dot(hidden, w_out, preferred_element_type=jnp.float32).astype(jnp.bfloat16)
    return pre_act, hidden, tower_out


def tower_back(row_block, w_out, pre_act, hidden, grad_out):
    dw_out = jnp.einsum("nf,nd->fd", hidden, grad_out, preferred_element_type=jnp.float32)
    grad_hidden = jnp.einsum("nd,fd->nf", grad_out, w_out, preferred_element_type=jnp.float32)
    gelu_back = jax.vjp(jax.nn.gelu, pre_act)[1]
    grad_pre = gelu_back(grad_hidden)[0].astype(jnp.bfloat16)
    dw_in = jnp.einsum("ne,nf->ef", row_block, grad_pre, preferred_element_type=jnp.float32)
    return grad_pre, dw_in, dw_out


def loss_grads(query, targ_vec, cand_vec, log_q, targ_ids, cand_ids, tok_total):
    logit_scale = SCORE_GAIN / math.sqrt(query.shape[1])
    z_targ = jnp.einsum("td,td->t", query, targ_vec, preferred_element_type=jnp.float32) * logit_scale
    z_cand = jnp.einsum("td,sd->ts", query, cand_vec, preferred_element_type=jnp.float32) * logit_scale - log_q[None, :]
    z_cand = jnp.where(targ_ids[:, None] == cand_ids[None, :], HIT_VALUE, z_cand)
    row_max = jnp.maximum(z_targ, jnp.max(z_cand, axis=1))
    e_targ = jnp.exp(z_targ - row_max)
    e_cand = jnp.exp(z_cand - row_max[:, None])
    denom_sum = e_targ + jnp.sum(e_cand, axis=1)
    loss_sum = jnp.sum(jnp.log(denom_sum) + row_max - z_targ)
    dz_targ = ((e_targ / denom_sum - 1.0) / tok_total).astype(jnp.bfloat16).astype(jnp.float32)
    dz_cand = (e_cand / denom_sum[:, None] / tok_total).astype(jnp.bfloat16)
    d_query = ((dz_targ[:, None] * targ_vec.astype(jnp.float32) + jnp.einsum("ts,sd->td", dz_cand, cand_vec, preferred_element_type=jnp.float32)) * logit_scale).astype(jnp.bfloat16)
    d_targ_vec = (logit_scale * dz_targ[:, None] * query.astype(jnp.float32)).astype(jnp.bfloat16)
    return loss_sum, d_query, d_targ_vec, dz_cand, logit_scale


def copy_to(src, dst, send_sem, recv_sem, dev):
    return pltpu.make_async_remote_copy(src, dst, send_sem, recv_sem, device_id=(dev,), device_id_type=MESH)


def all_to_all_body(n, src, dst, send_sem, recv_sem, own_sem):
    me = lax.axis_index("dp")
    barrier = pltpu.get_barrier_semaphore()

    def greet(i, carry):
        pl.semaphore_signal(barrier, inc=1, device_id=(lax.rem(me + i, n),), device_id_type=MESH)
        return carry

    lax.fori_loop(1, n, greet, 0)
    own = pltpu.make_async_copy(src.at[me], dst.at[me], own_sem)
    own.start()
    pl.semaphore_wait(barrier, n - 1)

    def send(i, carry):
        dev = lax.rem(me + i, n)
        copy_to(src.at[dev], dst.at[me], send_sem, recv_sem, dev).start()
        return carry

    lax.fori_loop(1, n, send, 0)
    own.wait()
    others = copy_to(src.at[pl.ds(0, n - 1)], dst.at[pl.ds(0, n - 1)], send_sem, recv_sem, me)
    others.wait_send()
    others.wait_recv()


def root_barrier(n, root, me):
    barrier = pltpu.get_barrier_semaphore()
    is_root = me // 2 == root

    def greet(i, carry):
        pl.semaphore_signal(barrier, inc=1, device_id=(lax.rem(me + i, n),), device_id_type=MESH)
        return carry

    @pl.when(is_root)
    def _():
        lax.fori_loop(1, n, greet, 0)
        pl.semaphore_wait(barrier, n - 1)

    @pl.when(jnp.logical_not(is_root))
    def _():
        for core in range(2):
            pl.semaphore_signal(barrier, inc=1, device_id=(2 * root + core,), device_id_type=MESH)
        pl.semaphore_wait(barrier, 2)

    return is_root


def scatter_body(n, root, src, dst, send_sem, recv_sem, own_sem):
    me = lax.axis_index("dp")
    is_root = root_barrier(n, root, me)

    def send(i, carry):
        dev = lax.rem(me + i, n)
        copy_to(src.at[dev], dst.at[lax.rem(me, 2)], send_sem, recv_sem, dev).start()
        return carry

    @pl.when(is_root)
    def _():
        lax.fori_loop(1, n, send, 0)
        own = pltpu.make_async_copy(src.at[me], dst.at[lax.rem(me, 2)], own_sem)
        own.start()
        own.wait()
        copy_to(src.at[pl.ds(0, n - 1)], src.at[pl.ds(0, n - 1)], send_sem, recv_sem, me).wait_send()
        copy_to(src.at[0], dst.at[0], send_sem, recv_sem, me).wait_recv()

    @pl.when(jnp.logical_not(is_root))
    def _():
        copy_to(src.at[pl.ds(0, 2)], dst, send_sem, recv_sem, me).wait_recv()


def gather_body(n, root, src, dst, send_sem, recv_sem, own_sem):
    me = lax.axis_index("dp")
    is_root = root_barrier(n, root, me)
    core = lax.rem(me, 2)
    partner = 2 * root + 1 - core

    @pl.when(is_root)
    def _():
        copy_to(src.at[1 - core], dst.at[me], send_sem, recv_sem, partner).start()
        own = pltpu.make_async_copy(src.at[core], dst.at[me], own_sem)
        own.start()
        own.wait()
        copy_to(src.at[0], dst.at[0], send_sem, recv_sem, me).wait_send()
        copy_to(dst.at[pl.ds(0, n - 1)], dst.at[pl.ds(0, n - 1)], send_sem, recv_sem, me).wait_recv()

    @pl.when(jnp.logical_not(is_root))
    def _():
        for to in range(2):
            copy_to(src.at[to], dst.at[me], send_sem, recv_sem, 2 * root + to).start()
        copy_to(src, src, send_sem, recv_sem, me).wait_send()


def comm_call(body, src, out_shape, collective_id, name, us, memory=ANY):
    return pl.pallas_call(
        body,
        out_shape=jax.ShapeDtypeStruct(out_shape, src.dtype),
        in_specs=[memory],
        out_specs=memory,
        scratch_shapes=[pltpu.SemaphoreType.DMA, pltpu.SemaphoreType.DMA, pltpu.SemaphoreType.DMA],
        compiler_params=pltpu.CompilerParams(collective_id=collective_id, has_side_effects=True),
        name=name,
    )(src)


def solution(mesh):
    n = mesh.shape["dp"]

    def local_step(tokens, w_one, w_two, wi_one, wi_two, table_loc, cand_ids, log_q, targ_loc):
        me = lax.axis_index("dp")
        rows_loc, width = table_loc.shape
        num_tok = tokens.shape[0]
        num_cand = cand_ids.shape[0]
        cand_loc = num_cand // n
        num_req = num_tok + cand_loc
        tok_total = num_tok * n

        def swap(src, collective_id, name):
            return comm_call(functools.partial(all_to_all_body, n), src, src.shape, collective_id, name, 50)

        req_ids = jnp.concatenate([targ_loc, lax.dynamic_slice(cand_ids, (me * cand_loc,), (cand_loc,))])
        owner = req_ids // rows_loc
        local_id = req_ids - owner * rows_loc
        is_owner = (owner[:, None] == jnp.arange(n)[None, :]).astype(jnp.bfloat16)
        earlier = (jnp.arange(num_req)[:, None] > jnp.arange(num_req)[None, :]).astype(jnp.bfloat16)
        before = jnp.dot(earlier, is_owner, preferred_element_type=jnp.float32)
        is_owner_f = is_owner.astype(jnp.float32)
        rank = jnp.sum(before * is_owner_f, axis=1).astype(jnp.int32)
        counts = jnp.sum(is_owner_f, axis=0).astype(jnp.int32)

        depth = -(-num_req // 128) * 128
        is_rank = (rank[:, None] == jnp.arange(depth)[None, :]).astype(jnp.bfloat16)
        place = jnp.arange(num_req)
        halves = [local_id // 64, local_id % 64, place // 64, place % 64, jnp.ones_like(place)]
        picks = jnp.concatenate([is_owner * h.astype(jnp.bfloat16)[:, None] for h in halves], axis=1)
        tables = jnp.einsum("ia,ij->aj", picks, is_rank, preferred_element_type=jnp.float32).astype(jnp.int32).reshape(5, n, depth)
        want_ids = jnp.where(tables[4] > 0, tables[0] * 64 + tables[1], -1)
        places = tables[2] * 64 + tables[3]

        lines = depth // 128
        note = jnp.concatenate([
            want_ids.reshape(n, lines, 128),
            jnp.broadcast_to(jnp.pad(counts, (0, 128 - n))[None, None, :], (n, 16 - lines, 128)),
        ], axis=1)
        notes = comm_call(functools.partial(all_to_all_body, n), note, note.shape, 0, "notes", 8)
        ask_ids = notes[:, :lines].reshape(n, depth)
        all_counts = notes[:, lines, :n]

        most = jnp.max(all_counts)
        too_many = most > PAIR_ROWS + HOT_ROWS
        extra_rounds = jnp.where(too_many, (most + PAIR_ROWS - 1) // PAIR_ROWS - 1, 0)
        hot_chip = jnp.max(all_counts.reshape(n, n // 2, 2), axis=(0, 2)) > PAIR_ROWS
        hot_chip = hot_chip & jnp.logical_not(too_many)
        num_hot = jnp.sum(hot_chip.astype(jnp.int32))
        hot_rank = jnp.sum((jnp.arange(n // 2)[None, :] < jnp.arange(n // 2)[:, None]) & hot_chip[None, :], axis=1)

        def hot_at(i):
            return jnp.sum(jnp.where(hot_chip & (hot_rank == i), jnp.arange(n // 2), 0))

        ask_pad = jnp.pad(ask_ids, ((0, 0), (0, HOT_ROWS)), constant_values=-1)
        place_pad = jnp.pad(places, ((0, 0), (0, HOT_ROWS)))

        def window(table, at, size):
            return lax.dynamic_slice(table, (0, at), (table.shape[0], size))

        def fetch(ids):
            picked = jnp.take(table_loc, jnp.maximum(ids.reshape(-1), 0), axis=0)
            return picked.reshape(ids.shape + (width,))

        def place_rows(rows, got, at, size, mine):
            inside = mine & (rank >= at) & (rank < at + size)
            slot = lax.rem(owner, got.shape[0]) * size + jnp.clip(rank - at, 0, size - 1)
            return jnp.where(inside[:, None], jnp.take(got.reshape(-1, width), slot, axis=0), rows)

        got = swap(fetch(ask_ids[:, :PAIR_ROWS]), 1, "rows_in")
        slot = owner * PAIR_ROWS + jnp.clip(rank, 0, PAIR_ROWS - 1)
        raw = jnp.take(got.reshape(-1, width), slot, axis=0)

        def extra_in(r, rows):
            got = swap(fetch(window(ask_pad, r * PAIR_ROWS, PAIR_ROWS)), 1, "rows_in")
            return place_rows(rows, got, r * PAIR_ROWS, PAIR_ROWS, True)

        raw = lax.fori_loop(1, 1 + extra_rounds, extra_in, raw)

        def hot_in(i, rows):
            chip = hot_at(i)
            hot_ids = ask_ids[:, PAIR_ROWS:PAIR_ROWS + HOT_ROWS]
            out = lax.cond(me // 2 == chip, lambda: fetch(hot_ids), lambda: jnp.zeros(hot_ids.shape + (width,), jnp.bfloat16))

            def from_root(root):
                return lambda src: comm_call(functools.partial(scatter_body, n, root), src, (2, HOT_ROWS, width), 2 + root, f"rows_in_{root}", 120)

            got = lax.switch(chip, [from_root(k) for k in range(n // 2)], out)
            return place_rows(rows, got, PAIR_ROWS, HOT_ROWS, owner // 2 == chip)

        raw = lax.fori_loop(0, num_hot, hot_in, raw)

        i_pre, i_hidden, i_vec = tower_fwd(raw, wi_one, wi_two)
        targ_vec, cand_vec_mine = i_vec[:num_tok], i_vec[num_tok:]
        cand_vec = lax.all_gather(cand_vec_mine, "dp", axis=0, tiled=True)
        q_pre, q_hidden, query = tower_fwd(tokens, w_one, w_two)
        loss_sum, d_query, d_targ_vec, dz_cand, logit_scale = loss_grads(query, targ_vec, cand_vec, log_q, targ_loc, cand_ids, tok_total)
        d_cand_part = jnp.einsum("ts,td->sd", dz_cand, query, preferred_element_type=jnp.float32)
        d_cand_vec = (lax.psum_scatter(d_cand_part, "dp", scatter_dimension=0, tiled=True) * logit_scale).astype(jnp.bfloat16)
        dw_one, dw_two = tower_back(tokens, w_two, q_pre, q_hidden, d_query)[1:]
        d_vec = jnp.concatenate([d_targ_vec, d_cand_vec])
        i_grad_pre, dwi_one, dwi_two = tower_back(raw, wi_two, i_pre, i_hidden, d_vec)
        d_raw = jnp.einsum("nf,df->nd", i_grad_pre, wi_one, preferred_element_type=jnp.float32).astype(jnp.bfloat16)
        weight_grads = lax.psum((dw_one, dw_two, dwi_one, dwi_two), "dp")
        loss = lax.psum(loss_sum, "dp") / tok_total

        def spread(ids):
            return jnp.take(d_raw, ids.reshape(-1), axis=0).reshape(ids.shape + (width,))

        def add_rows(acc, ids, rows):
            ids = ids.reshape(-1)
            ids = jnp.where(ids >= 0, ids, rows_loc)
            return acc.at[ids].add(rows.reshape(-1, width).astype(jnp.float32), mode="drop")

        back = swap(spread(places[:, :PAIR_ROWS]), 1, "rows_out")
        d_table = add_rows(jnp.zeros((rows_loc, width), jnp.float32), ask_ids[:, :PAIR_ROWS], back)

        def extra_out(r, acc):
            back = swap(spread(window(place_pad, r * PAIR_ROWS, PAIR_ROWS)), 1, "rows_out")
            return add_rows(acc, window(ask_pad, r * PAIR_ROWS, PAIR_ROWS), back)

        d_table = lax.fori_loop(1, 1 + extra_rounds, extra_out, d_table)

        def hot_out(i, acc):
            chip = hot_at(i)
            hot_places = lax.dynamic_slice(places, (2 * chip, PAIR_ROWS), (2, HOT_ROWS))

            def to_root(root):
                return lambda src: comm_call(functools.partial(gather_body, n, root), src, (n, HOT_ROWS, width), 2 + n // 2 + root, f"rows_out_{root}", 120)

            back = lax.switch(chip, [to_root(k) for k in range(n // 2)], spread(hot_places))
            hot_ids = ask_ids[:, PAIR_ROWS:PAIR_ROWS + HOT_ROWS]
            return lax.cond(me // 2 == chip, lambda a: add_rows(a, hot_ids, back), lambda a: a, acc)

        d_table = lax.fori_loop(0, num_hot, hot_out, d_table)
        return (loss, d_table) + tuple(weight_grads)

    return jax.shard_map(local_step, mesh=mesh, in_specs=(P("dp", None), P(), P(), P(), P(), P("dp", None), P(), P(), P("dp")), out_specs=(P(), P("dp", None), P(), P(), P(), P()), check_vma=False)
```

```python
import functools
import math
import jax
import jax.numpy as jnp
from jax import lax
from jax.experimental import pallas as pl
from jax.experimental.pallas import tpu as pltpu
from jax.sharding import PartitionSpec as P

SCORE_GAIN = 3.0
HIT_VALUE = -1e9
PAIR_ROWS = 48
HOT_ROWS = 240
CHUNKS = 128
LAG = 3
MESH = pl.DeviceIdType.MESH
ANY = pl.BlockSpec(memory_space=pl.ANY)


def tower_fwd(row_block, w_in, w_out):
    pre_act = jnp.dot(row_block, w_in, preferred_element_type=jnp.float32)
    hidden = jax.nn.gelu(pre_act).astype(jnp.bfloat16)
    tower_out = jnp.dot(hidden, w_out, preferred_element_type=jnp.float32).astype(jnp.bfloat16)
    return pre_act, hidden, tower_out


def tower_back(row_block, w_out, pre_act, hidden, grad_out):
    dw_out = jnp.einsum("nf,nd->fd", hidden, grad_out, preferred_element_type=jnp.float32)
    grad_hidden = jnp.einsum("nd,fd->nf", grad_out, w_out, preferred_element_type=jnp.float32)
    gelu_back = jax.vjp(jax.nn.gelu, pre_act)[1]
    grad_pre = gelu_back(grad_hidden)[0].astype(jnp.bfloat16)
    dw_in_t = jnp.einsum("nf,ne->fe", grad_pre, row_block, preferred_element_type=jnp.float32)
    return grad_pre, dw_in_t, dw_out


def loss_grads(query, targ_vec, cand_vec, log_q, targ_ids, cand_ids, tok_total):
    logit_scale = SCORE_GAIN / math.sqrt(query.shape[1])
    z_targ = jnp.einsum("td,td->t", query, targ_vec, preferred_element_type=jnp.float32) * logit_scale
    z_cand = jnp.einsum("td,sd->ts", query, cand_vec, preferred_element_type=jnp.float32) * logit_scale - log_q[None, :]
    z_cand = jnp.where(targ_ids[:, None] == cand_ids[None, :], HIT_VALUE, z_cand)
    row_max = jnp.maximum(z_targ, jnp.max(z_cand, axis=1))
    e_targ = jnp.exp(z_targ - row_max)
    e_cand = jnp.exp(z_cand - row_max[:, None])
    denom_sum = e_targ + jnp.sum(e_cand, axis=1)
    loss_sum = jnp.sum(jnp.log(denom_sum) + row_max - z_targ)
    dz_targ = ((e_targ / denom_sum - 1.0) / tok_total).astype(jnp.bfloat16).astype(jnp.float32)
    dz_cand = (e_cand / denom_sum[:, None] / tok_total).astype(jnp.bfloat16)
    d_query = ((dz_targ[:, None] * targ_vec.astype(jnp.float32) + jnp.einsum("ts,sd->td", dz_cand, cand_vec, preferred_element_type=jnp.float32)) * logit_scale).astype(jnp.bfloat16)
    d_targ_vec = (logit_scale * dz_targ[:, None] * query.astype(jnp.float32)).astype(jnp.bfloat16)
    return loss_sum, d_query, d_targ_vec, dz_cand, logit_scale


def copy_to(src, dst, send_sem, recv_sem, dev):
    return pltpu.make_async_remote_copy(src, dst, send_sem, recv_sem, device_id=(dev,), device_id_type=MESH)


def all_to_all_body(n, src, dst, send_sem, recv_sem, own_sem):
    me = lax.axis_index("dp")
    barrier = pltpu.get_barrier_semaphore()

    def greet(i, carry):
        pl.semaphore_signal(barrier, inc=1, device_id=(lax.rem(me + i, n),), device_id_type=MESH)
        return carry

    lax.fori_loop(1, n, greet, 0)
    own = pltpu.make_async_copy(src.at[me], dst.at[me], own_sem)
    own.start()
    pl.semaphore_wait(barrier, n - 1)

    def send(i, carry):
        dev = lax.rem(me + i, n)
        copy_to(src.at[dev], dst.at[me], send_sem, recv_sem, dev).start()
        return carry

    lax.fori_loop(1, n, send, 0)
    own.wait()
    others = copy_to(src.at[pl.ds(0, n - 1)], dst.at[pl.ds(0, n - 1)], send_sem, recv_sem, me)
    others.wait_send()
    others.wait_recv()


def root_barrier(n, root, me):
    barrier = pltpu.get_barrier_semaphore()
    is_root = me // 2 == root

    def greet(i, carry):
        pl.semaphore_signal(barrier, inc=1, device_id=(lax.rem(me + i, n),), device_id_type=MESH)
        return carry

    @pl.when(is_root)
    def _():
        lax.fori_loop(1, n, greet, 0)
        pl.semaphore_wait(barrier, n - 1)

    @pl.when(jnp.logical_not(is_root))
    def _():
        for core in range(2):
            pl.semaphore_signal(barrier, inc=1, device_id=(2 * root + core,), device_id_type=MESH)
        pl.semaphore_wait(barrier, 2)

    return is_root


TREES = (
    ((4368, 13104, 273, 224), (17476, 52425, 1092, 0), (43689, 2, 2730, 0)),
    ((4353, 13059, 284, 528), (17476, 52380, 1088, 64), (43674, 32, 2720, 160)),
)


def tree_depths(masks, start, chips):
    depth = {start: 0}
    while len(depth) < chips:
        for c, at in tuple(depth.items()):
            for d, to in enumerate((c ^ 1, c ^ 2, c + 4, c - 4)):
                if masks[d] >> c & 1:
                    depth[to] = at + 1
    return depth


def broadcast_body(n, root, src, dst, send_sem, recv_sem, pair_send, pair_recv, echo_send, echo_recv):
    me = lax.axis_index("dp")
    core = lax.rem(me, 2)
    chip = me // 2
    at_x, at_y, at_z = lax.rem(chip, 2), lax.rem(chip // 2, 2), chip // 4
    root_z = root // 4
    up = 1 if root_z < 2 else -1
    rel_z = at_z if root_z < 2 else 3 - at_z
    rel = (rel_z * 2 + lax.rem(at_y + root // 2, 2)) * 2 + lax.rem(at_x + root, 2)
    is_root = chip == root
    trees = TREES[min(root_z, 3 - root_z)]
    to = (me + 2 - 4 * at_x, me + 4 - 8 * at_y, me + 8 * up, me - 8 * up)
    partner = me + 1 - 2 * core

    def passes(mask):
        hit = rel < 0
        for c in range(n // 2):
            if mask >> c & 1:
                hit = hit | (rel == c)
        return hit

    moves = [[(d, passes(trees[t][d])) for d in range(4) if trees[t][d]] for t in range(3)]
    depths = [tree_depths(trees[t], 4 * min(root_z, 3 - root_z), n // 2) for t in range(3)]
    behind = [LAG * sum((rel == c).astype(jnp.int32) * depths[t][c] for c in range(n // 2)) for t in range(3)]

    barrier = pltpu.get_barrier_semaphore()
    for dev in (to[0], to[1], partner):
        pl.semaphore_signal(barrier, inc=1, device_id=(dev,), device_id_type=MESH)
    has_up, has_down = at_z < n // 8 - 1, at_z > 0

    @pl.when(has_up)
    def _():
        pl.semaphore_signal(barrier, inc=1, device_id=(me + 8,), device_id_type=MESH)

    @pl.when(has_down)
    def _():
        pl.semaphore_signal(barrier, inc=1, device_id=(me - 8,), device_id_type=MESH)

    pl.semaphore_wait(barrier, 3 + has_up.astype(jnp.int32) + has_down.astype(jnp.int32))

    rows = src.shape[0] // CHUNKS
    steps = -(-CHUNKS // 3)

    def step(held, j, t):
        piece = pl.ds((3 * j + t) * rows, rows)
        for d, on in moves[t]:
            @pl.when(on)
            def _():
                copy_to(held.at[piece], dst.at[core, piece], send_sem.at[t, d], recv_sem.at[t, j], to[d]).start()

    @pl.when(is_root)
    def _():
        copy_to(src, dst.at[core], pair_send, pair_recv, partner).start()

        def go(j, carry):
            for t in range(3):
                pl.when(3 * j + t < CHUNKS)(functools.partial(step, src, j, t))
            return carry

        lax.fori_loop(0, steps, go, 0)
        copy_to(src, dst.at[1 - core], pair_send, pair_recv, partner).wait_recv()
        copy_to(dst.at[1 - core], dst.at[1 - core], echo_send, echo_recv, partner).start()
        copy_to(dst.at[core], dst.at[core], echo_send, echo_recv, partner).wait()

    @pl.when(jnp.logical_not(is_root))
    def _():
        held = dst.at[core]

        def relay(t, j):
            piece = pl.ds((3 * j + t) * rows, rows)
            copy_to(held.at[piece], held.at[piece], send_sem.at[t, 0], recv_sem.at[t, j], me).wait_recv()
            step(held, j, t)
            copy_to(held.at[piece], dst.at[core, piece], pair_send, pair_recv, partner).start()

        def go(i, carry):
            for t in range(3):
                j = i - behind[t]
                pl.when((j >= 0) & (3 * j + t < CHUNKS))(functools.partial(relay, t, j))
            return carry

        far = max(max(d.values()) for d in depths)
        lax.fori_loop(LAG, steps + LAG * far, go, 0)
        copy_to(held, dst.at[1 - core], pair_send, pair_recv, partner).wait_recv()

    copy_to(src, dst.at[core], pair_send, pair_recv, partner).wait_send()
    for t in range(3):
        part = pl.ds(0, len(range(t, CHUNKS, 3)) * rows)
        for d, on in moves[t]:
            @pl.when(on)
            def _():
                copy_to(src.at[part], dst.at[core, part], send_sem.at[t, d], recv_sem.at[t, 0], me).wait_send()


def gather_body(n, root, src, dst, send_sem, recv_sem, own_sem):
    me = lax.axis_index("dp")
    is_root = root_barrier(n, root, me)
    core = lax.rem(me, 2)
    partner = 2 * root + 1 - core

    @pl.when(is_root)
    def _():
        copy_to(src.at[1 - core], dst.at[me], send_sem, recv_sem, partner).start()
        own = pltpu.make_async_copy(src.at[core], dst.at[me], own_sem)
        own.start()
        own.wait()
        copy_to(src.at[0], dst.at[0], send_sem, recv_sem, me).wait_send()
        copy_to(dst.at[pl.ds(0, n - 1)], dst.at[pl.ds(0, n - 1)], send_sem, recv_sem, me).wait_recv()

    @pl.when(jnp.logical_not(is_root))
    def _():
        for to in range(2):
            copy_to(src.at[to], dst.at[me], send_sem, recv_sem, 2 * root + to).start()
        copy_to(src, src, send_sem, recv_sem, me).wait_send()


X, Y, Z1, Z2 = 2, 4, 8, 16
PARTS = ((0, 512, (X, Y, Z1, Z2)), (512, 512, (Y, X, Z1, Z2)), (1024, 256, (Z1, X, Y, Z2)), (1280, 256, (Z1, Y, X, Z2)))
GROUP = 1536


def sum_body(n, groups, srcs, note, out, note_out, acc, got, notes, load_sem, pair_sem, half_sem, full_sem, send_sem, out_sem, note_sem):
    me = lax.axis_index("dp")
    core = lax.rem(me, 2)
    partner = me + 1 - 2 * core
    bit = {d: lax.rem(me // d, 2) for d in (X, Y, Z1, Z2)}
    across = {d: me + d * (1 - 2 * bit[d]) for d in bit}
    per_src = srcs[0].shape[0] // GROUP
    full = got[0]

    def spot(part, level):
        start, rows, dims = part
        at, size = start // 2, rows // 2
        for d in dims[:level]:
            size //= 2
            at = at + bit[d] * size
        return at if level == 0 else pl.multiple_of(at, 8), size

    def away(part, level):
        at, size = spot(part, level)
        return pl.multiple_of(at + (1 - bit[part[2][level]]) * (size // 2), 8), size // 2

    barrier = pltpu.get_barrier_semaphore()

    def greet(i, carry):
        pl.semaphore_signal(barrier, inc=1, device_id=(lax.rem(me + i, n),), device_id_type=MESH)
        return carry

    lax.fori_loop(1, n, greet, 0)
    for g in range(groups):
        src, base = srcs[g // per_src], g % per_src * GROUP
        for start, rows, _ in PARTS:
            half = rows // 2
            mine = src.at[pl.ds(pl.multiple_of(base + start + core * half, 8), half)]
            pltpu.make_async_copy(mine, acc.at[g, pl.ds(start // 2, half)], load_sem.at[g]).start()
    notes[me] = note[...]
    pl.semaphore_wait(barrier, n - 1)

    for g in range(groups):
        src, base = srcs[g // per_src], g % per_src * GROUP
        for start, rows, _ in PARTS:
            half = rows // 2
            other = src.at[pl.ds(pl.multiple_of(base + start + (1 - core) * half, 8), half)]
            copy_to(other, full.at[g, pl.ds(start // 2, half)], send_sem.at[0], pair_sem.at[g], partner).start()

    def tell(i, carry):
        copy_to(note, notes.at[me], note_sem.at[0], note_sem.at[1], lax.rem(me + i, n)).start()
        return carry

    lax.fori_loop(1, n, tell, 0)

    def add(dst, at, x, x_at, y, y_at, size, g):
        block = min(size, 32)

        def one(i, carry):
            k = pl.multiple_of(i * block, block)
            dst[g, pl.ds(at + k, block)] = x[g, pl.ds(x_at + k, block)] + y[g, pl.ds(y_at + k, block)]
            return carry

        lax.fori_loop(0, size // block, one, 0)

    def advance(stage, g):
        if stage == 0:
            pltpu.make_async_copy(acc.at[g], acc.at[g], load_sem.at[g]).wait()
            copy_to(full.at[g], full.at[g], send_sem.at[0], pair_sem.at[g], me).wait_recv()
        for p, part in enumerate(PARTS):
            start, rows, dims = part
            if stage <= 4:
                at, size = spot(part, stage)
                in_at = start >> (stage + 1)
                arrived = got[stage].at[g, pl.ds(in_at, size)]
                if stage:
                    copy_to(arrived, arrived, send_sem.at[0], half_sem.at[stage - 1, p, g], me).wait_recv()
                if stage < 4:
                    add(acc, at, acc, at, got[stage], in_at, size, g)
                    off, half = away(part, stage)
                    copy_to(acc.at[g, pl.ds(off, half)], got[stage + 1].at[g, pl.ds(start >> (stage + 2), half)],
                            send_sem.at[stage + 1], half_sem.at[stage, p, g], across[dims[stage]]).start()
                    continue
                add(full, at, acc, at, got[stage], in_at, size, g)
            else:
                back_at, back = spot(part, 9 - stage)
                there = full.at[g, pl.ds(pl.multiple_of(back_at + (1 - 2 * bit[dims[8 - stage]]) * back, 8), back)]
                copy_to(there, there, send_sem.at[0], full_sem.at[stage - 5, p, g], me).wait_recv()
                at, size = spot(part, 8 - stage)
            if stage < 8:
                held = full.at[g, pl.ds(at, size)]
                copy_to(held, held, send_sem.at[stage + 1], full_sem.at[stage - 4, p, g], across[dims[7 - stage]]).start()
            else:
                half = rows // 2
                held = full.at[g, pl.ds(start // 2, half)]
                place = out.at[pl.ds(pl.multiple_of(g * GROUP + start + core * half, 8), half)]
                copy_to(held, place, send_sem.at[9], out_sem.at[0], partner).start()
                pltpu.make_async_copy(held, place, out_sem.at[1]).start()

    def tick(k, carry):
        for stage in reversed(range(9)):
            g = k - stage
            pl.when((g >= 0) & (g < groups))(functools.partial(advance, stage, g))
        return carry

    lax.fori_loop(0, groups + 8, tick, 0)

    others = copy_to(notes.at[pl.ds(0, n - 1)], notes.at[pl.ds(0, n - 1)], note_sem.at[0], note_sem.at[1], me)
    others.wait_send()
    others.wait_recv()
    note_out[...] = jnp.sum(notes[...], axis=0)
    for i, sent in enumerate((0, 1, 2, 3, 4, 4, 3, 2, 1, 0)):
        copy_to(got[sent], got[sent], send_sem.at[i], out_sem.at[0], me).wait_send()
    half_out = out.at[pl.ds(0, groups * GROUP // 2)]
    copy_to(half_out, half_out, send_sem.at[0], out_sem.at[0], me).wait_recv()
    pltpu.make_async_copy(half_out, half_out, out_sem.at[1]).wait()


def sum_over_devices(n, srcs, note, collective_id):
    rows, width = srcs[0].shape
    groups = len(srcs) * rows // GROUP
    sizes = [(groups, GROUP // 2 >> i, width) for i in range(5)]

    def body(*refs):
        k = len(srcs)
        ins, note_in, out, note_out = refs[:k], refs[k], refs[k + 1], refs[k + 2]
        acc, got, rest = refs[k + 3], refs[k + 4:k + 9], refs[k + 9:]
        sum_body(n, groups, ins, note_in, out, note_out, acc, got, *rest)

    vmem = pl.BlockSpec(memory_space=pltpu.VMEM)
    dma = pltpu.SemaphoreType.DMA
    return pl.pallas_call(
        body,
        out_shape=(jax.ShapeDtypeStruct((len(srcs) * rows, width), jnp.float32), jax.ShapeDtypeStruct(note.shape, jnp.float32)),
        in_specs=[ANY] * len(srcs) + [vmem],
        out_specs=(ANY, vmem),
        scratch_shapes=[pltpu.VMEM(sizes[0], jnp.float32)] + [pltpu.VMEM(s, jnp.float32) for s in sizes] + [
            pltpu.VMEM((n,) + note.shape, jnp.float32),
            dma((groups,)), dma((groups,)), dma((4, len(PARTS), groups)), dma((4, len(PARTS), groups)), dma((10,)), dma((2,)), dma((2,)),
        ],
        compiler_params=pltpu.CompilerParams(collective_id=collective_id, has_side_effects=True, vmem_limit_bytes=40 << 20 if groups <= 4 else 62 << 20),
        cost_estimate=pl.CostEstimate(flops=200 * 30_000_000, bytes_accessed=0, transcendentals=0),
        name="weight_sums",
    )(*srcs, note)


def comm_call(body, src, out_shape, collective_id, name, sems=((), (), ()), us=50):
    return pl.pallas_call(
        body,
        out_shape=jax.ShapeDtypeStruct(out_shape, src.dtype),
        in_specs=[ANY],
        out_specs=ANY,
        scratch_shapes=[pltpu.SemaphoreType.DMA(shape) if shape else pltpu.SemaphoreType.DMA for shape in sems],
        compiler_params=pltpu.CompilerParams(collective_id=collective_id, has_side_effects=True),
        cost_estimate=pl.CostEstimate(flops=us * 30_000_000, bytes_accessed=0, transcendentals=0),
        name=name,
    )(src)


def solution(mesh):
    n = mesh.shape["dp"]

    def local_step(tokens, w_one, w_two, wi_one, wi_two, table_loc, cand_ids, log_q, targ_loc):
        me = lax.axis_index("dp")
        rows_loc, width = table_loc.shape
        num_tok = tokens.shape[0]
        num_cand = cand_ids.shape[0]
        cand_loc = num_cand // n
        num_req = num_tok + cand_loc
        tok_total = num_tok * n

        def swap(src, collective_id, name):
            return comm_call(functools.partial(all_to_all_body, n), src, src.shape, collective_id, name)

        cand_at = cand_ids - me * rows_loc
        cand_here = (cand_at >= 0) & (cand_at < rows_loc)
        cand_rows = jnp.where(cand_here[:, None], jnp.take(table_loc, jnp.clip(cand_at, 0, rows_loc - 1), axis=0), 0)
        cand_mine = lax.psum_scatter(cand_rows, "dp", scatter_dimension=0, tiled=True)
        cand_vec_mine = tower_fwd(cand_mine, wi_one, wi_two)[2]

        req_ids = jnp.concatenate([targ_loc, lax.dynamic_slice(cand_ids, (me * cand_loc,), (cand_loc,))])
        owner = req_ids // rows_loc
        local_id = req_ids - owner * rows_loc
        is_owner = (owner[:, None] == jnp.arange(n)[None, :]).astype(jnp.bfloat16)
        earlier = (jnp.arange(num_req)[:, None] > jnp.arange(num_req)[None, :]).astype(jnp.bfloat16)
        before = jnp.dot(earlier, is_owner, preferred_element_type=jnp.float32)
        is_owner_f = is_owner.astype(jnp.float32)
        rank = jnp.sum(before * is_owner_f, axis=1).astype(jnp.int32)
        counts = jnp.sum(is_owner_f, axis=0).astype(jnp.int32)

        depth = -(-num_req // 128) * 128
        is_rank = (rank[:, None] == jnp.arange(depth)[None, :]).astype(jnp.bfloat16)
        place = jnp.arange(num_req)
        halves = [local_id // 64, local_id % 64, place // 64, place % 64, jnp.ones_like(place)]
        picks = jnp.concatenate([is_owner * h.astype(jnp.bfloat16)[:, None] for h in halves], axis=1)
        tables = jnp.einsum("ia,ij->aj", picks, is_rank, preferred_element_type=jnp.float32).astype(jnp.int32).reshape(5, n, depth)
        want_ids = jnp.where(tables[4] > 0, tables[0] * 64 + tables[1], -1)
        places = tables[2] * 64 + tables[3]

        lines = depth // 128
        note = jnp.concatenate([
            want_ids.reshape(n, lines, 128),
            jnp.broadcast_to(jnp.pad(counts, (0, 128 - n))[None, None, :], (n, 16 - lines, 128)),
        ], axis=1)
        notes = comm_call(functools.partial(all_to_all_body, n), note, note.shape, 0, "notes")
        ask_ids = notes[:, :lines].reshape(n, depth)
        all_counts = notes[:, lines, :n]

        most = jnp.max(all_counts)
        too_many = most > PAIR_ROWS + HOT_ROWS
        extra_rounds = jnp.where(too_many, (most + PAIR_ROWS - 1) // PAIR_ROWS - 1, 0)
        hot_chip = jnp.max(all_counts.reshape(n, n // 2, 2), axis=(0, 2)) > PAIR_ROWS
        num_hot = jnp.sum(hot_chip.astype(jnp.int32))
        hot_rank = jnp.sum((jnp.arange(n // 2)[None, :] < jnp.arange(n // 2)[:, None]) & hot_chip[None, :], axis=1)

        def hot_at(i):
            return jnp.sum(jnp.where(hot_chip & (hot_rank == i), jnp.arange(n // 2), 0))

        ask_pad = jnp.pad(ask_ids, ((0, 0), (0, HOT_ROWS)), constant_values=-1)
        place_pad = jnp.pad(places, ((0, 0), (0, HOT_ROWS)))

        def window(table, at, size):
            return lax.dynamic_slice(table, (0, at), (table.shape[0], size))

        def fetch(ids):
            picked = jnp.take(table_loc, jnp.maximum(ids.reshape(-1), 0), axis=0)
            return picked.reshape(ids.shape + (width,))

        def hot_in(i, rows):
            chip = hot_at(i)

            def from_root(root):
                sems = ((3, 4), (3, -(-CHUNKS // 3)), (), (), (), ())
                return lambda src: comm_call(functools.partial(broadcast_body, n, root), src, (2, rows_loc, width), 2 + root, f"rows_in_{root}", sems)

            got = lax.switch(chip, [from_root(k) for k in range(n // 2)], table_loc)
            found = jnp.take(got.reshape(-1, width), lax.rem(owner, 2) * rows_loc + local_id, axis=0)
            return jnp.where((owner // 2 == chip)[:, None], found, rows)

        hot_raw = lax.fori_loop(0, num_hot, hot_in, jnp.zeros((num_req, width), jnp.bfloat16))
        rows_out = fetch(ask_ids[:, :PAIR_ROWS])
        hot_raw, cand_vec_mine, rows_out = lax.optimization_barrier((hot_raw, cand_vec_mine, rows_out))
        cand_vec = lax.all_gather(cand_vec_mine, "dp", axis=0, tiled=True)
        got = swap(rows_out, 1, "rows_in")
        slot = owner * PAIR_ROWS + jnp.clip(rank, 0, PAIR_ROWS - 1)
        from_hot = jnp.any((owner[:, None] // 2 == jnp.arange(n // 2)[None, :]) & hot_chip[None, :], axis=1)
        raw = jnp.where(from_hot[:, None], hot_raw, jnp.take(got.reshape(-1, width), slot, axis=0))

        i_pre, i_hidden, i_vec = tower_fwd(raw, wi_one, wi_two)
        targ_vec = i_vec[:num_tok]
        q_pre, q_hidden, query = tower_fwd(tokens, w_one, w_two)
        loss_sum, d_query, d_targ_vec, dz_cand, logit_scale = loss_grads(query, targ_vec, cand_vec, log_q, targ_loc, cand_ids, tok_total)
        d_cand_part = jnp.einsum("ts,td->sd", dz_cand, query, preferred_element_type=jnp.float32)
        d_cand_vec = (lax.psum_scatter(d_cand_part, "dp", scatter_dimension=0, tiled=True) * logit_scale).astype(jnp.bfloat16)
        dw_one_t, dw_two = tower_back(tokens, w_two, q_pre, q_hidden, d_query)[1:]
        query_sums = lax.psum((dw_one_t, dw_two), "dp")
        d_vec = jnp.concatenate([d_targ_vec, d_cand_vec])
        i_grad_pre, dwi_one_t, dwi_two = tower_back(raw, wi_two, i_pre, i_hidden, d_vec)
        d_raw = jnp.einsum("nf,df->nd", i_grad_pre, wi_one, preferred_element_type=jnp.float32).astype(jnp.bfloat16)
        loss_note = jnp.full((8, 128), loss_sum, jnp.float32)
        item_sums, loss_note = sum_over_devices(n, (dwi_one_t, dwi_two), loss_note, 2 + n)
        item_sums, d_raw = lax.optimization_barrier((item_sums, d_raw))
        loss = loss_note[0, 0] / tok_total
        dwi_one, dwi_two = item_sums[:item_sums.shape[0] // 2].T, item_sums[item_sums.shape[0] // 2:]

        def spread(ids):
            return jnp.take(d_raw, ids.reshape(-1), axis=0).reshape(ids.shape + (width,))

        def add_rows(acc, ids, rows):
            ids = ids.reshape(-1)
            ids = jnp.where(ids >= 0, ids, rows_loc)
            return acc.at[ids].add(rows.reshape(-1, width).astype(jnp.float32), mode="drop")

        back = swap(spread(places[:, :PAIR_ROWS]), 1, "rows_out")
        d_table = add_rows(jnp.zeros((rows_loc, width), jnp.float32), ask_ids[:, :PAIR_ROWS], back)

        def extra_out(r, acc):
            back = swap(spread(window(place_pad, r * PAIR_ROWS, PAIR_ROWS)), 1, "rows_out")
            return add_rows(acc, window(ask_pad, r * PAIR_ROWS, PAIR_ROWS), back)

        d_table = lax.fori_loop(1, 1 + extra_rounds, extra_out, d_table)

        def hot_out(i, acc):
            chip = hot_at(i)
            hot_places = lax.dynamic_slice(places, (2 * chip, PAIR_ROWS), (2, HOT_ROWS))

            def to_root(root):
                return lambda src: comm_call(functools.partial(gather_body, n, root), src, (n, HOT_ROWS, width), 2 + n // 2 + root, f"rows_out_{root}")

            back = lax.switch(chip, [to_root(k) for k in range(n // 2)], spread(hot_places))
            hot_ids = ask_ids[:, PAIR_ROWS:PAIR_ROWS + HOT_ROWS]
            return lax.cond(me // 2 == chip, lambda a: add_rows(a, hot_ids, back), lambda a: a, acc)

        d_table = lax.fori_loop(0, jnp.where(too_many, 0, num_hot), hot_out, d_table)
        return loss, d_table, query_sums[0].T, query_sums[1], dwi_one, dwi_two

    return jax.shard_map(local_step, mesh=mesh, in_specs=(P("dp", None), P(), P(), P(), P(), P("dp", None), P(), P(), P("dp")), out_specs=(P(), P("dp", None), P(), P(), P(), P()), check_vma=False)
```

```python
import functools
import math
import jax
import jax.numpy as jnp
from jax import lax
from jax.experimental import pallas as pl
from jax.experimental.pallas import tpu as pltpu
from jax.sharding import PartitionSpec as P

SCORE_GAIN = 3.0
HIT_VALUE = -1e9
PAIR_ROWS = 48
HOT_ROWS = 240
SLICES = 5
CHUNKS = 128
LAG = 3
MESH = pl.DeviceIdType.MESH
ANY = pl.BlockSpec(memory_space=pl.ANY)


def tower_fwd(row_block, w_in, w_out):
    pre_act = jnp.dot(row_block, w_in, preferred_element_type=jnp.float32)
    hidden = jax.nn.gelu(pre_act).astype(jnp.bfloat16)
    tower_out = jnp.dot(hidden, w_out, preferred_element_type=jnp.float32).astype(jnp.bfloat16)
    return pre_act, hidden, tower_out


def tower_back(row_block, w_out, pre_act, hidden, grad_out):
    dw_out = jnp.einsum("nf,nd->fd", hidden, grad_out, preferred_element_type=jnp.float32)
    grad_hidden = jnp.einsum("nd,fd->nf", grad_out, w_out, preferred_element_type=jnp.float32)
    gelu_back = jax.vjp(jax.nn.gelu, pre_act)[1]
    grad_pre = gelu_back(grad_hidden)[0].astype(jnp.bfloat16)
    dw_in_t = jnp.einsum("nf,ne->fe", grad_pre, row_block, preferred_element_type=jnp.float32)
    return grad_pre, dw_in_t, dw_out


def loss_grads(query, targ_vec, cand_vec, log_q, targ_ids, cand_ids, tok_total):
    logit_scale = SCORE_GAIN / math.sqrt(query.shape[1])
    z_targ = jnp.einsum("td,td->t", query, targ_vec, preferred_element_type=jnp.float32) * logit_scale
    z_cand = jnp.einsum("td,sd->ts", query, cand_vec, preferred_element_type=jnp.float32) * logit_scale - log_q[None, :]
    z_cand = jnp.where(targ_ids[:, None] == cand_ids[None, :], HIT_VALUE, z_cand)
    row_max = jnp.maximum(z_targ, jnp.max(z_cand, axis=1))
    e_targ = jnp.exp(z_targ - row_max)
    e_cand = jnp.exp(z_cand - row_max[:, None])
    denom_sum = e_targ + jnp.sum(e_cand, axis=1)
    loss_sum = jnp.sum(jnp.log(denom_sum) + row_max - z_targ)
    dz_targ = ((e_targ / denom_sum - 1.0) / tok_total).astype(jnp.bfloat16).astype(jnp.float32)
    dz_cand = (e_cand / denom_sum[:, None] / tok_total).astype(jnp.bfloat16)
    d_query = ((dz_targ[:, None] * targ_vec.astype(jnp.float32) + jnp.einsum("ts,sd->td", dz_cand, cand_vec, preferred_element_type=jnp.float32)) * logit_scale).astype(jnp.bfloat16)
    d_targ_vec = (logit_scale * dz_targ[:, None] * query.astype(jnp.float32)).astype(jnp.bfloat16)
    return loss_sum, d_query, d_targ_vec, dz_cand, logit_scale


def copy_to(src, dst, send_sem, recv_sem, dev):
    return pltpu.make_async_remote_copy(src, dst, send_sem, recv_sem, device_id=(dev,), device_id_type=MESH)


def greet(*devs):
    barrier = pltpu.get_barrier_semaphore()
    for dev in devs:
        pl.semaphore_signal(barrier, device_id=(dev,), device_id_type=MESH)
    return barrier


def each_other(n, me, act):
    def one(i, carry):
        act(lax.rem(me + i, n))
        return carry

    lax.fori_loop(1, n, one, None)


def arrived(ref, sem):
    copy_to(ref, ref, sem, sem, lax.axis_index("dp")).wait_recv()


def departed(ref, sem):
    copy_to(ref, ref, sem, sem, lax.axis_index("dp")).wait_send()


def all_to_all_body(n, src, dst, send_sem, recv_sem, own_sem):
    me = lax.axis_index("dp")
    each_other(n, me, greet)
    barrier = greet()
    own = pltpu.make_async_copy(src.at[me], dst.at[me], own_sem)
    own.start()
    pl.semaphore_wait(barrier, n - 1)

    each_other(n, me, lambda dev: copy_to(src.at[dev], dst.at[me], send_sem, recv_sem, dev).start())
    own.wait()
    departed(src.at[pl.ds(0, n - 1)], send_sem)
    arrived(dst.at[pl.ds(0, n - 1)], recv_sem)


def root_barrier(n, root, me):
    is_root = me // 2 == root

    @pl.when(is_root)
    def _():
        each_other(n, me, greet)
        pl.semaphore_wait(greet(), n - 1)

    @pl.when(jnp.logical_not(is_root))
    def _():
        pl.semaphore_wait(greet(2 * root, 2 * root + 1), 2)

    return is_root


TREES = (
    ((4368, 13104, 273, 224), (17476, 52425, 1092, 0), (43689, 2, 2730, 0)),
    ((4353, 13059, 284, 528), (17476, 52380, 1088, 64), (43674, 32, 2720, 160)),
)


def tree_depths(masks, start, chips):
    depth = {start: 0}
    while len(depth) < chips:
        for c, at in tuple(depth.items()):
            for d, to in enumerate((c ^ 1, c ^ 2, c + 4, c - 4)):
                if masks[d] >> c & 1:
                    depth[to] = at + 1
    return depth


def broadcast_body(n, root, src, dst, send_sem, recv_sem, pair_send, pair_recv, echo_send, echo_recv):
    me = lax.axis_index("dp")
    core = lax.rem(me, 2)
    chip = me // 2
    at_x, at_y, at_z = lax.rem(chip, 2), lax.rem(chip // 2, 2), chip // 4
    root_z = root // 4
    up = 1 if root_z < 2 else -1
    rel_z = at_z if root_z < 2 else 3 - at_z
    rel = (rel_z * 2 + lax.rem(at_y + root // 2, 2)) * 2 + lax.rem(at_x + root, 2)
    is_root = chip == root
    trees = TREES[min(root_z, 3 - root_z)]
    to = (me + 2 - 4 * at_x, me + 4 - 8 * at_y, me + 8 * up, me - 8 * up)
    partner = me + 1 - 2 * core

    def passes(mask):
        hit = rel < 0
        for c in range(n // 2):
            if mask >> c & 1:
                hit = hit | (rel == c)
        return hit

    moves = [[(d, passes(trees[t][d])) for d in range(4) if trees[t][d]] for t in range(3)]
    depths = [tree_depths(trees[t], 4 * min(root_z, 3 - root_z), n // 2) for t in range(3)]
    behind = [LAG * sum((rel == c).astype(jnp.int32) * depths[t][c] for c in range(n // 2)) for t in range(3)]

    barrier = greet(to[0], to[1], partner)
    has_up, has_down = at_z < n // 8 - 1, at_z > 0

    @pl.when(has_up)
    def _():
        greet(me + 8)

    @pl.when(has_down)
    def _():
        greet(me - 8)

    pl.semaphore_wait(barrier, 3 + has_up.astype(jnp.int32) + has_down.astype(jnp.int32))

    rows = src.shape[0] // CHUNKS
    steps = -(-CHUNKS // 3)

    def step(held, j, t):
        piece = pl.ds((3 * j + t) * rows, rows)
        for d, on in moves[t]:
            @pl.when(on)
            def _():
                copy_to(held.at[piece], dst.at[core, piece], send_sem.at[t, d], recv_sem.at[t, j], to[d]).start()

    @pl.when(is_root)
    def _():
        copy_to(src, dst.at[core], pair_send, pair_recv, partner).start()

        def go(j, carry):
            for t in range(3):
                pl.when(3 * j + t < CHUNKS)(functools.partial(step, src, j, t))
            return carry

        lax.fori_loop(0, steps, go, None)
        arrived(dst.at[1 - core], pair_recv)
        copy_to(dst.at[1 - core], dst.at[1 - core], echo_send, echo_recv, partner).start()
        copy_to(dst.at[core], dst.at[core], echo_send, echo_recv, partner).wait()

    @pl.when(jnp.logical_not(is_root))
    def _():
        held = dst.at[core]

        def relay(t, j):
            piece = pl.ds((3 * j + t) * rows, rows)
            arrived(held.at[piece], recv_sem.at[t, j])
            step(held, j, t)
            copy_to(held.at[piece], dst.at[core, piece], pair_send, pair_recv, partner).start()

        def go(i, carry):
            for t in range(3):
                j = i - behind[t]
                pl.when((j >= 0) & (3 * j + t < CHUNKS))(functools.partial(relay, t, j))
            return carry

        far = max(max(d.values()) for d in depths)
        lax.fori_loop(LAG, steps + LAG * far, go, None)
        arrived(held, pair_recv)

    departed(src, pair_send)
    for t in range(3):
        part = pl.ds(0, len(range(t, CHUNKS, 3)) * rows)
        for d, on in moves[t]:
            @pl.when(on)
            def _():
                departed(src.at[part], send_sem.at[t, d])


def gather_add_body(n, root, src, ids, table, table_out, rows, acc, send_sem, recv_sem, own_sem, load_sem):
    me = lax.axis_index("dp")
    is_root = root_barrier(n, root, me)
    core = lax.rem(me, 2)
    partner = 2 * root + 1 - core
    slices, _, size, width = src.shape
    block, depth, wide = 1024, 512, 256
    blocks, deeps, wides = acc.shape[0] // block, n * size // depth, width // wide
    mine = pl.ds(pl.multiple_of(me * size, size), size)

    @pl.when(is_root)
    def _():
        load = pltpu.make_async_copy(table, acc, load_sem)
        load.start()
        for k in range(slices):
            copy_to(src.at[k, 1 - core], rows.at[k, mine], send_sem, recv_sem.at[k], partner).start()
            pltpu.make_async_copy(src.at[k, core], rows.at[k, mine], own_sem.at[k]).start()
        load.wait()

        def take(k, carry):
            arrived(rows.at[k, pl.ds(0, (n - 1) * size)], recv_sem.at[k])
            pltpu.make_async_copy(src.at[k, core], rows.at[k, mine], own_sem.at[k]).wait()

            def add(i, carry):
                b, d, w = lax.rem(i // wides, blocks), i // (wides * blocks), lax.rem(i, wides)
                at = pl.multiple_of(b * block, block)
                deep = pl.ds(pl.multiple_of(d * depth, depth), depth)
                columns = pl.ds(pl.multiple_of(w * wide, wide), wide)
                row = lax.broadcasted_iota(jnp.int32, (block, depth), 0) + at
                pick = (row == ids[k, :, deep]).astype(jnp.float32).astype(jnp.bfloat16)
                acc[pl.ds(at, block), columns] += jnp.dot(pick, rows[k, deep, columns], preferred_element_type=jnp.float32)
                return carry

            return lax.fori_loop(0, blocks * deeps * wides, add, carry)

        lax.fori_loop(0, slices, take, None)
        store = pltpu.make_async_copy(acc, table_out, load_sem)
        store.start()
        store.wait()
        departed(src.at[:, 0], send_sem)

    @pl.when(jnp.logical_not(is_root))
    def _():
        for k in range(slices):
            for to in range(2):
                copy_to(src.at[k, to], rows.at[k, mine], send_sem, recv_sem.at[k], 2 * root + to).start()
        departed(src, send_sem)


def gather_add(n, root, src, ids, table, collective_id):
    slices, _, size, width = src.shape
    dma = pltpu.SemaphoreType.DMA
    return pl.pallas_call(
        functools.partial(gather_add_body, n, root),
        out_shape=jax.ShapeDtypeStruct(table.shape, table.dtype),
        in_specs=[ANY, pl.BlockSpec(memory_space=pltpu.VMEM), ANY],
        out_specs=ANY,
        input_output_aliases={2: 0},
        scratch_shapes=[pltpu.VMEM((slices, n * size, width), src.dtype), pltpu.VMEM(table.shape, table.dtype), dma, dma((slices,)), dma((slices,)), dma],
        compiler_params=pltpu.CompilerParams(collective_id=collective_id, has_side_effects=True, vmem_limit_bytes=40 << 20),
        cost_estimate=pl.CostEstimate(flops=150 * 30_000_000, bytes_accessed=0, transcendentals=0),
        name=f"rows_out_{root}",
    )(src, ids, table)


CAND_PARTS = ((0, 24, (3, 2, 1, 0)), (24, 24, (2, 3, 1, 0)), (48, 8, (1, 3, 2, 0)), (56, 8, (1, 2, 3, 0)))


def cand_sum_body(n, src, out, *refs):
    num = len(CAND_PARTS)
    acc, refs = refs[:num], refs[num:]
    got, (load_sem, recv_sem, send_sem) = [refs[i * num:(i + 1) * num] for i in range(5)], refs[5 * num:]
    me = lax.axis_index("dp")
    core = lax.rem(me, 2)
    bit = [lax.rem(me // d, 2) for d in (16, 8, 4, 2)]
    across = [me + d * (1 - 2 * b) for d, b in zip((16, 8, 4, 2), bit)]
    partner = me + 1 - 2 * core
    every = slice(None)

    pl.semaphore_wait(greet(partner, *across), 5)

    for p, (at, rows, _) in enumerate(CAND_PARTS):
        w = pl.ds(at, rows)
        copy_to(src.at[:, :, :, :, 1 - core, w], got[0][p], send_sem.at[0, p], recv_sem.at[0, p], partner).start()
        pltpu.make_async_copy(src.at[:, :, :, :, core, w], acc[p], load_sem.at[p]).start()

    def add(p, level, fixed):
        held = CAND_PARTS[p][2][:level]
        free = [a for a in range(4) if fixed[a] is every]
        for k in range(2 ** len(free)):
            index = list(fixed)
            for j, a in enumerate(free):
                index[a] = k >> j & 1
            there = tuple(index[a] for a in range(4) if a not in held)
            acc[p][tuple(index)] += got[level][p][there]

    for level in range(5):
        for p, (at, rows, dims) in enumerate(CAND_PARTS):
            if level == 0:
                pltpu.make_async_copy(acc[p], acc[p], load_sem.at[p]).wait()
            arrived(got[level][p], recv_sem.at[level, p])
            fixed = [bit[a] if a in dims[:level] else every for a in range(4)]
            if level == 4:
                out[pl.ds(at, rows)] = acc[p][tuple(fixed)] + got[4][p][...]
                continue
            axis = dims[level]
            away, kept = list(fixed), list(fixed)
            away[axis], kept[axis] = 1 - bit[axis], bit[axis]
            add(p, level, away)
            copy_to(acc[p].at[tuple(away)], got[level + 1][p], send_sem.at[level + 1, p], recv_sem.at[level + 1, p], across[axis]).start()
            add(p, level, kept)
    for level in range(5):
        for p in range(num):
            departed(got[level][p], send_sem.at[level, p])


def cand_sum(n, part, collective_id):
    width = part.shape[1]
    dma = pltpu.SemaphoreType.DMA
    sizes = [[(2,) * (4 - level) + (rows, width) for _, rows, _ in CAND_PARTS] for level in range(5)]
    return pl.pallas_call(
        functools.partial(cand_sum_body, n),
        out_shape=jax.ShapeDtypeStruct((part.shape[0] // n, width), part.dtype),
        in_specs=[ANY],
        out_specs=pl.BlockSpec(memory_space=pltpu.VMEM),
        scratch_shapes=[pltpu.VMEM(s, part.dtype) for level in [0] + list(range(5)) for s in sizes[level]] + [dma((len(CAND_PARTS),)), dma((5, len(CAND_PARTS))), dma((5, len(CAND_PARTS)))],
        compiler_params=pltpu.CompilerParams(collective_id=collective_id, has_side_effects=True, vmem_limit_bytes=20 << 20),
        cost_estimate=pl.CostEstimate(flops=40 * 30_000_000, bytes_accessed=0, transcendentals=0),
        name="cand_sums",
    )(part.reshape(2, 2, 2, 2, 2, part.shape[0] // n, width))


X, Y, Z1, Z2 = 2, 4, 8, 16
PARTS = ((0, 512, (X, Y, Z1, Z2)), (512, 512, (Y, X, Z1, Z2)), (1024, 256, (Z1, X, Y, Z2)), (1280, 256, (Z1, Y, X, Z2)))
GROUP = 1536


def sum_body(n, groups, srcs, note, outs, note_out, acc, got, notes, load_sem, pair_sem, half_sem, full_sem, send_sem, out_sem, note_sem):
    me = lax.axis_index("dp")
    core = lax.rem(me, 2)
    partner = me + 1 - 2 * core
    bit = {d: lax.rem(me // d, 2) for d in (X, Y, Z1, Z2)}
    across = {d: me + d * (1 - 2 * bit[d]) for d in bit}
    per_src = srcs[0].shape[0] // GROUP
    full = got[0]

    def spot(part, level):
        start, rows, dims = part
        at, size = start // 2, rows // 2
        for d in dims[:level]:
            size //= 2
            at = at + bit[d] * size
        return at if level == 0 else pl.multiple_of(at, 8), size

    def away(part, level):
        at, size = spot(part, level)
        return pl.multiple_of(at + (1 - bit[part[2][level]]) * (size // 2), 8), size // 2

    each_other(n, me, greet)
    for g in range(groups):
        src, base = srcs[g // per_src], g % per_src * GROUP
        for start, rows, _ in PARTS:
            half = rows // 2
            mine = src.at[pl.ds(pl.multiple_of(base + start + core * half, 8), half)]
            pltpu.make_async_copy(mine, acc.at[g, pl.ds(start // 2, half)], load_sem.at[g]).start()
    notes[me] = note[...]
    pl.semaphore_wait(greet(), n - 1)

    for g in range(groups):
        src, base = srcs[g // per_src], g % per_src * GROUP
        for start, rows, _ in PARTS:
            half = rows // 2
            other = src.at[pl.ds(pl.multiple_of(base + start + (1 - core) * half, 8), half)]
            copy_to(other, full.at[g, pl.ds(start // 2, half)], send_sem.at[0], pair_sem.at[g], partner).start()

    each_other(n, me, lambda dev: copy_to(note, notes.at[me], note_sem.at[0], note_sem.at[1], dev).start())

    def add(dst, at, x, x_at, y, y_at, size, g):
        block = min(size, 32)

        def one(i, carry):
            k = pl.multiple_of(i * block, block)
            dst[g, pl.ds(at + k, block)] = x[g, pl.ds(x_at + k, block)] + y[g, pl.ds(y_at + k, block)]
            return carry

        lax.fori_loop(0, size // block, one, None)

    def advance(stage, g):
        if stage == 0:
            pltpu.make_async_copy(acc.at[g], acc.at[g], load_sem.at[g]).wait()
            arrived(full.at[g], pair_sem.at[g])
        for p, part in enumerate(PARTS):
            start, rows, dims = part
            if stage <= 4:
                at, size = spot(part, stage)
                in_at = start >> (stage + 1)
                if stage:
                    arrived(got[stage].at[g, pl.ds(in_at, size)], half_sem.at[stage - 1, p, g])
                if stage < 4:
                    add(acc, at, acc, at, got[stage], in_at, size, g)
                    off, half = away(part, stage)
                    copy_to(acc.at[g, pl.ds(off, half)], got[stage + 1].at[g, pl.ds(start >> (stage + 2), half)],
                            send_sem.at[stage + 1], half_sem.at[stage, p, g], across[dims[stage]]).start()
                    continue
                add(full, at, acc, at, got[stage], in_at, size, g)
            else:
                back_at, back = spot(part, 9 - stage)
                there = full.at[g, pl.ds(pl.multiple_of(back_at + (1 - 2 * bit[dims[8 - stage]]) * back, 8), back)]
                arrived(there, full_sem.at[stage - 5, p, g])
                at, size = spot(part, 8 - stage)
            if stage < 8:
                held = full.at[g, pl.ds(at, size)]
                copy_to(held, held, send_sem.at[stage + 1], full_sem.at[stage - 4, p, g], across[dims[7 - stage]]).start()
            else:
                half = rows // 2
                held = full.at[g, pl.ds(start // 2, half)]
                place = pl.ds(pl.multiple_of(lax.rem(g, per_src) * GROUP + start + core * half, 8), half)
                for i, out in enumerate(outs):
                    @pl.when(g // per_src == i)
                    def _():
                        copy_to(held, out.at[place], send_sem.at[9], out_sem.at[0], partner).start()
                        pltpu.make_async_copy(held, out.at[place], out_sem.at[1]).start()

    def tick(k, carry):
        for stage in reversed(range(9)):
            g = k - stage
            pl.when((g >= 0) & (g < groups))(functools.partial(advance, stage, g))
        return carry

    lax.fori_loop(0, groups + 8, tick, None)

    departed(notes.at[pl.ds(0, n - 1)], note_sem.at[0])
    arrived(notes.at[pl.ds(0, n - 1)], note_sem.at[1])
    note_out[...] = jnp.sum(notes[...], axis=0)
    for i, sent in enumerate(got):
        departed(sent, send_sem.at[i])
        departed(sent, send_sem.at[9 - i])
    arrived(full, out_sem.at[0])
    pltpu.make_async_copy(full, full, out_sem.at[1]).wait()


def sum_over_devices(n, srcs, note, collective_id):
    rows, width = srcs[0].shape
    groups = len(srcs) * rows // GROUP
    sizes = [(groups, GROUP // 2 >> i, width) for i in range(5)]

    def body(*refs):
        rest = iter(refs)
        ins, note_in = [next(rest) for _ in srcs], next(rest)
        outs, note_out = [next(rest) for _ in srcs], next(rest)
        acc, got = next(rest), [next(rest) for _ in sizes]
        sum_body(n, groups, ins, note_in, outs, note_out, acc, got, *rest)

    vmem = pl.BlockSpec(memory_space=pltpu.VMEM)
    dma = pltpu.SemaphoreType.DMA
    return pl.pallas_call(
        body,
        out_shape=tuple(jax.ShapeDtypeStruct(x.shape, jnp.float32) for x in tuple(srcs) + (note,)),
        in_specs=[ANY] * len(srcs) + [vmem],
        out_specs=(ANY,) * len(srcs) + (vmem,),
        scratch_shapes=[pltpu.VMEM(sizes[0], jnp.float32)] + [pltpu.VMEM(s, jnp.float32) for s in sizes] + [
            pltpu.VMEM((n,) + note.shape, jnp.float32),
            dma((groups,)), dma((groups,)), dma((4, len(PARTS), groups)), dma((4, len(PARTS), groups)), dma((10,)), dma((2,)), dma((2,)),
        ],
        compiler_params=pltpu.CompilerParams(collective_id=collective_id, has_side_effects=True, vmem_limit_bytes=40 << 20),
        cost_estimate=pl.CostEstimate(flops=200 * 30_000_000, bytes_accessed=0, transcendentals=0),
        name="weight_sums",
    )(*srcs, note)


def comm_call(body, src, out_shape, collective_id, name, sems=((), (), ()), us=50):
    return pl.pallas_call(
        body,
        out_shape=jax.ShapeDtypeStruct(out_shape, src.dtype),
        in_specs=[ANY],
        out_specs=ANY,
        scratch_shapes=[pltpu.SemaphoreType.DMA(shape) if shape else pltpu.SemaphoreType.DMA for shape in sems],
        compiler_params=pltpu.CompilerParams(collective_id=collective_id, has_side_effects=True),
        cost_estimate=pl.CostEstimate(flops=us * 30_000_000, bytes_accessed=0, transcendentals=0),
        name=name,
    )(src)


def solution(mesh):
    n = mesh.shape["dp"]

    def local_step(tokens, w_one, w_two, wi_one, wi_two, table_loc, cand_ids, log_q, targ_loc):
        me = lax.axis_index("dp")
        rows_loc, width = table_loc.shape
        num_tok = tokens.shape[0]
        num_cand = cand_ids.shape[0]
        cand_loc = num_cand // n
        num_req = num_tok + cand_loc
        tok_total = num_tok * n

        def swap(src, collective_id, name):
            return comm_call(functools.partial(all_to_all_body, n), src, src.shape, collective_id, name)

        cand_at = cand_ids - me * rows_loc
        cand_here = (cand_at >= 0) & (cand_at < rows_loc)
        cand_rows = jnp.where(cand_here[:, None], jnp.take(table_loc, jnp.clip(cand_at, 0, rows_loc - 1), axis=0), 0)
        cand_mine = lax.psum_scatter(cand_rows, "dp", scatter_dimension=0, tiled=True)
        cand_vec_mine = tower_fwd(cand_mine, wi_one, wi_two)[2]

        req_ids = jnp.concatenate([targ_loc, lax.dynamic_slice(cand_ids, (me * cand_loc,), (cand_loc,))])
        owner = req_ids // rows_loc
        local_id = req_ids - owner * rows_loc
        is_owner = (owner[:, None] == jnp.arange(n)[None, :]).astype(jnp.bfloat16)
        earlier = (jnp.arange(num_req)[:, None] > jnp.arange(num_req)[None, :]).astype(jnp.bfloat16)
        before = jnp.dot(earlier, is_owner, preferred_element_type=jnp.float32)
        is_owner_f = is_owner.astype(jnp.float32)
        rank = jnp.sum(before * is_owner_f, axis=1).astype(jnp.int32)
        counts = jnp.sum(is_owner_f, axis=0).astype(jnp.int32)

        depth = -(-num_req // 128) * 128
        is_rank = (rank[:, None] == jnp.arange(depth)[None, :]).astype(jnp.bfloat16)
        place = jnp.arange(num_req)
        halves = [local_id // 64, local_id % 64, place // 64, place % 64, jnp.ones_like(place)]
        picks = jnp.concatenate([is_owner * h.astype(jnp.bfloat16)[:, None] for h in halves], axis=1)
        tables = jnp.einsum("ia,ij->aj", picks, is_rank, preferred_element_type=jnp.float32).astype(jnp.int32).reshape(5, n, depth)
        want_ids = jnp.where(tables[4] > 0, tables[0] * 64 + tables[1], -1)
        places = tables[2] * 64 + tables[3]

        lines = depth // 128
        note = jnp.concatenate([
            want_ids.reshape(n, lines, 128),
            jnp.broadcast_to(jnp.pad(counts, (0, 128 - n))[None, None, :], (n, 16 - lines, 128)),
        ], axis=1)
        notes = comm_call(functools.partial(all_to_all_body, n), note, note.shape, 0, "notes")
        ask_ids = notes[:, :lines].reshape(n, depth)
        all_counts = notes[:, lines, :n]

        most = jnp.max(all_counts)
        too_many = most > PAIR_ROWS + HOT_ROWS
        extra_rounds = jnp.where(too_many, (most + PAIR_ROWS - 1) // PAIR_ROWS - 1, 0)
        hot_chip = jnp.max(all_counts.reshape(n, n // 2, 2), axis=(0, 2)) > PAIR_ROWS
        num_hot = jnp.sum(hot_chip.astype(jnp.int32))
        hot_rank = jnp.sum((jnp.arange(n // 2)[None, :] < jnp.arange(n // 2)[:, None]) & hot_chip[None, :], axis=1)

        def hot_at(i):
            return jnp.sum(jnp.where(hot_chip & (hot_rank == i), jnp.arange(n // 2), 0))

        ask_pad = jnp.pad(ask_ids, ((0, 0), (0, HOT_ROWS)), constant_values=-1)
        place_pad = jnp.pad(places, ((0, 0), (0, HOT_ROWS)))

        def window(table, at, size):
            return lax.dynamic_slice(table, (0, at), (table.shape[0], size))

        def fetch(ids):
            picked = jnp.take(table_loc, jnp.maximum(ids.reshape(-1), 0), axis=0)
            return picked.reshape(ids.shape + (width,))

        def hot_in(i, rows):
            chip = hot_at(i)

            def from_root(root):
                sems = ((3, 4), (3, -(-CHUNKS // 3)), (), (), (), ())
                return lambda src: comm_call(functools.partial(broadcast_body, n, root), src, (2, rows_loc, width), 2 + root, f"rows_in_{root}", sems)

            got = lax.switch(chip, [from_root(k) for k in range(n // 2)], table_loc)
            found = jnp.take(got.reshape(-1, width), lax.rem(owner, 2) * rows_loc + local_id, axis=0)
            return jnp.where((owner // 2 == chip)[:, None], found, rows)

        hot_raw = lax.fori_loop(0, num_hot, hot_in, jnp.zeros((num_req, width), jnp.bfloat16))
        rows_out = fetch(ask_ids[:, :PAIR_ROWS])
        hot_raw, cand_vec_mine, rows_out = lax.optimization_barrier((hot_raw, cand_vec_mine, rows_out))
        cand_vec = lax.all_gather(cand_vec_mine, "dp", axis=0, tiled=True)
        got = swap(rows_out, 1, "rows_in")
        slot = owner * PAIR_ROWS + jnp.clip(rank, 0, PAIR_ROWS - 1)
        from_hot = jnp.any((owner[:, None] // 2 == jnp.arange(n // 2)[None, :]) & hot_chip[None, :], axis=1)
        raw = jnp.where(from_hot[:, None], hot_raw, jnp.take(got.reshape(-1, width), slot, axis=0))

        i_pre, i_hidden, i_vec = tower_fwd(raw, wi_one, wi_two)
        targ_vec = i_vec[:num_tok]
        q_pre, q_hidden, query = tower_fwd(tokens, w_one, w_two)
        loss_sum, d_query, d_targ_vec, dz_cand, logit_scale = loss_grads(query, targ_vec, cand_vec, log_q, targ_loc, cand_ids, tok_total)
        d_cand_part = jnp.einsum("ts,td->sd", dz_cand, query, preferred_element_type=jnp.float32)
        dw_one_t, dw_two = tower_back(tokens, w_two, q_pre, q_hidden, d_query)[1:]
        d_cand_part, dw_one_t, dw_two = lax.optimization_barrier((d_cand_part, dw_one_t, dw_two))
        query_sums = lax.psum((dw_one_t, dw_two), "dp")
        d_cand_vec = (cand_sum(n, d_cand_part, 3 + n) * logit_scale).astype(jnp.bfloat16)
        d_vec = jnp.concatenate([d_targ_vec, d_cand_vec])
        i_grad_pre, dwi_one_t, dwi_two = tower_back(raw, wi_two, i_pre, i_hidden, d_vec)
        d_raw = jnp.einsum("nf,df->nd", i_grad_pre, wi_one, preferred_element_type=jnp.float32).astype(jnp.bfloat16)
        def spread(ids):
            return jnp.take(d_raw, ids.reshape(-1), axis=0).reshape(ids.shape + (width,))

        def add_rows(acc, ids, rows):
            ids = ids.reshape(-1)
            ids = jnp.where(ids >= 0, ids, rows_loc)
            return acc.at[ids].add(rows.reshape(-1, width).astype(jnp.float32), mode="drop")

        back = swap(spread(places[:, :PAIR_ROWS]), 1, "rows_out")
        d_table = add_rows(jnp.zeros((rows_loc, width), jnp.float32), ask_ids[:, :PAIR_ROWS], back)

        def extra_out(r, acc):
            back = swap(spread(window(place_pad, r * PAIR_ROWS, PAIR_ROWS)), 1, "rows_out")
            return add_rows(acc, window(ask_pad, r * PAIR_ROWS, PAIR_ROWS), back)

        d_table = lax.fori_loop(1, 1 + extra_rounds, extra_out, d_table)

        hot_ids = ask_ids[:, PAIR_ROWS:PAIR_ROWS + HOT_ROWS].reshape(n, SLICES, HOT_ROWS // SLICES)
        hot_ids = hot_ids.transpose(1, 0, 2).reshape(SLICES, 1, n * HOT_ROWS // SLICES)

        def hot_out(i, acc):
            chip = hot_at(i)
            hot_places = lax.dynamic_slice(places, (2 * chip, PAIR_ROWS), (2, HOT_ROWS))
            hot_places = hot_places.reshape(2, SLICES, HOT_ROWS // SLICES).transpose(1, 0, 2)

            def to_root(root):
                return lambda src, acc: gather_add(n, root, src, hot_ids, acc, 2 + n // 2 + root)

            return lax.switch(chip, [to_root(k) for k in range(n // 2)], spread(hot_places), acc)

        d_table = lax.fori_loop(0, jnp.where(too_many, 0, num_hot), hot_out, d_table)
        loss_note, d_table = lax.optimization_barrier((jnp.full((8, 128), loss_sum, jnp.float32), d_table))
        dwi_one_t, dwi_two, loss_note = sum_over_devices(n, (dwi_one_t, dwi_two), loss_note, 2 + n)
        loss = loss_note[0, 0] / tok_total
        return loss, d_table, query_sums[0].T, query_sums[1], dwi_one_t.T, dwi_two

    return jax.shard_map(local_step, mesh=mesh, in_specs=(P("dp", None), P(), P(), P(), P(), P("dp", None), P(), P(), P("dp")), out_specs=(P(), P("dp", None), P(), P(), P(), P()), check_vma=False)
```

```python
import functools
import math
import jax
import jax.numpy as jnp
from jax import lax
from jax.experimental import pallas as pl
from jax.experimental.pallas import tpu as pltpu
from jax.sharding import PartitionSpec as P

SCORE_GAIN = 3.0
HIT_VALUE = -1e9
PAIR_ROWS = 48
HOT_ROWS = 240
SLICES = 5
CHUNKS = 128
LAG = 3
MESH = pl.DeviceIdType.MESH
ANY = pl.BlockSpec(memory_space=pl.ANY)


def tower_fwd(row_block, w_in, w_out):
    pre_act = jnp.dot(row_block, w_in, preferred_element_type=jnp.float32)
    hidden = jax.nn.gelu(pre_act).astype(jnp.bfloat16)
    tower_out = jnp.dot(hidden, w_out, preferred_element_type=jnp.float32).astype(jnp.bfloat16)
    return pre_act, hidden, tower_out


def tower_back(row_block, w_out, pre_act, hidden, grad_out):
    dw_out = jnp.einsum("nf,nd->fd", hidden, grad_out, preferred_element_type=jnp.float32)
    grad_hidden = jnp.einsum("nd,fd->nf", grad_out, w_out, preferred_element_type=jnp.float32)
    gelu_back = jax.vjp(jax.nn.gelu, pre_act)[1]
    grad_pre = gelu_back(grad_hidden)[0].astype(jnp.bfloat16)
    dw_in = jnp.einsum("ne,nf->ef", row_block, grad_pre, preferred_element_type=jnp.float32)
    return grad_pre, dw_in, dw_out


def loss_grads(query, targ_vec, cand_vec, log_q, targ_ids, cand_ids, tok_total):
    logit_scale = SCORE_GAIN / math.sqrt(query.shape[1])
    z_targ = jnp.einsum("td,td->t", query, targ_vec, preferred_element_type=jnp.float32) * logit_scale
    z_cand = jnp.einsum("td,sd->ts", query, cand_vec, preferred_element_type=jnp.float32) * logit_scale - log_q[None, :]
    z_cand = jnp.where(targ_ids[:, None] == cand_ids[None, :], HIT_VALUE, z_cand)
    row_max = jnp.maximum(z_targ, jnp.max(z_cand, axis=1))
    e_targ = jnp.exp(z_targ - row_max)
    e_cand = jnp.exp(z_cand - row_max[:, None])
    denom_sum = e_targ + jnp.sum(e_cand, axis=1)
    loss_sum = jnp.sum(jnp.log(denom_sum) + row_max - z_targ)
    dz_targ = ((e_targ / denom_sum - 1.0) / tok_total).astype(jnp.bfloat16).astype(jnp.float32)
    dz_cand = (e_cand / denom_sum[:, None] / tok_total).astype(jnp.bfloat16)
    d_query = ((dz_targ[:, None] * targ_vec.astype(jnp.float32) + jnp.einsum("ts,sd->td", dz_cand, cand_vec, preferred_element_type=jnp.float32)) * logit_scale).astype(jnp.bfloat16)
    d_targ_vec = (logit_scale * dz_targ[:, None] * query.astype(jnp.float32)).astype(jnp.bfloat16)
    return loss_sum, d_query, d_targ_vec, dz_cand, logit_scale


def copy_to(src, dst, send_sem, recv_sem, dev):
    return pltpu.make_async_remote_copy(src, dst, send_sem, recv_sem, device_id=(dev,), device_id_type=MESH)


def greet(*devs):
    barrier = pltpu.get_barrier_semaphore()
    for dev in devs:
        pl.semaphore_signal(barrier, device_id=(dev,), device_id_type=MESH)
    return barrier


def each_other(n, me, act):
    def one(i, carry):
        act(lax.rem(me + i, n))
        return carry

    lax.fori_loop(1, n, one, None)


def arrived(ref, sem):
    copy_to(ref, ref, sem, sem, lax.axis_index("dp")).wait_recv()


def departed(ref, sem):
    copy_to(ref, ref, sem, sem, lax.axis_index("dp")).wait_send()


def swap_start(n, me, src, dst, send_sem, recv_sem, own_sem):
    pltpu.make_async_copy(src.at[me], dst.at[me], own_sem).start()
    each_other(n, me, lambda dev: copy_to(src.at[dev], dst.at[me], send_sem, recv_sem, dev).start())


def swap_end(n, me, src, dst, send_sem, recv_sem, own_sem):
    pltpu.make_async_copy(src.at[me], dst.at[me], own_sem).wait()
    departed(src.at[pl.ds(0, n - 1)], send_sem)
    arrived(dst.at[pl.ds(0, n - 1)], recv_sem)


def all_to_all_body(n, src, dst, *sems):
    me = lax.axis_index("dp")
    each_other(n, me, greet)
    pl.semaphore_wait(greet(), n - 1)
    swap_start(n, me, src, dst, *sems)
    swap_end(n, me, src, dst, *sems)


TREES = (
    ((4368, 13104, 273, 224), (17476, 52425, 1092, 0), (43689, 2, 2730, 0)),
    ((4353, 13059, 284, 528), (17476, 52380, 1088, 64), (43674, 32, 2720, 160)),
)


def tree_depths(masks, start, chips):
    depth = {start: 0}
    while len(depth) < chips:
        for c, at in tuple(depth.items()):
            for d, to in enumerate((c ^ 1, c ^ 2, c + 4, c - 4)):
                if masks[d] >> c & 1:
                    depth[to] = at + 1
    return depth


def rows_in_body(n, root, src, table, dst, blocks, send_sem, recv_sem, own_sem, *sems):
    me = lax.axis_index("dp")
    each_other(n, me, greet)
    pl.semaphore_wait(greet(), n - 1)
    swap_start(n, me, src, dst, send_sem, recv_sem, own_sem)
    if root < n // 2:
        broadcast(n, root, table, blocks, *sems)
    swap_end(n, me, src, dst, send_sem, recv_sem, own_sem)


def broadcast(n, root, src, dst, send_sem, recv_sem, pair_send, pair_recv, echo_send, echo_recv):
    me = lax.axis_index("dp")
    core = lax.rem(me, 2)
    chip = me // 2
    at_x, at_y, at_z = lax.rem(chip, 2), lax.rem(chip // 2, 2), chip // 4
    root_z = root // 4
    up = 1 if root_z < 2 else -1
    rel_z = at_z if root_z < 2 else 3 - at_z
    rel = (rel_z * 2 + lax.rem(at_y + root // 2, 2)) * 2 + lax.rem(at_x + root, 2)
    is_root = chip == root
    trees = TREES[min(root_z, 3 - root_z)]
    to = (me + 2 - 4 * at_x, me + 4 - 8 * at_y, me + 8 * up, me - 8 * up)
    partner = me + 1 - 2 * core

    def passes(mask):
        hit = rel < 0
        for c in range(n // 2):
            if mask >> c & 1:
                hit = hit | (rel == c)
        return hit

    moves = [[(d, passes(trees[t][d])) for d in range(4) if trees[t][d]] for t in range(3)]
    depths = [tree_depths(trees[t], 4 * min(root_z, 3 - root_z), n // 2) for t in range(3)]
    behind = [LAG * sum((rel == c).astype(jnp.int32) * depths[t][c] for c in range(n // 2)) for t in range(3)]

    rows = src.shape[0] // CHUNKS
    steps = -(-CHUNKS // 3)

    def step(held, j, t):
        piece = pl.ds((3 * j + t) * rows, rows)
        for d, on in moves[t]:
            @pl.when(on)
            def _():
                copy_to(held.at[piece], dst.at[core, piece], send_sem.at[t, d], recv_sem.at[t, j], to[d]).start()

    @pl.when(is_root)
    def _():
        copy_to(src, dst.at[core], pair_send, pair_recv, partner).start()

        def go(j, carry):
            for t in range(3):
                pl.when(3 * j + t < CHUNKS)(functools.partial(step, src, j, t))
            return carry

        lax.fori_loop(0, steps, go, None)
        arrived(dst.at[1 - core], pair_recv)
        copy_to(dst.at[1 - core], dst.at[1 - core], echo_send, echo_recv, partner).start()
        copy_to(dst.at[core], dst.at[core], echo_send, echo_recv, partner).wait()

    @pl.when(jnp.logical_not(is_root))
    def _():
        held = dst.at[core]

        def relay(t, j):
            piece = pl.ds((3 * j + t) * rows, rows)
            arrived(held.at[piece], recv_sem.at[t, j])
            step(held, j, t)
            copy_to(held.at[piece], dst.at[core, piece], pair_send, pair_recv, partner).start()

        def go(i, carry):
            for t in range(3):
                j = i - behind[t]
                pl.when((j >= 0) & (3 * j + t < CHUNKS))(functools.partial(relay, t, j))
            return carry

        far = max(max(d.values()) for d in depths)
        lax.fori_loop(LAG, steps + LAG * far, go, None)
        arrived(held, pair_recv)

    departed(src, pair_send)
    for t in range(3):
        part = pl.ds(0, len(range(t, CHUNKS, 3)) * rows)
        for d, on in moves[t]:
            @pl.when(on)
            def _():
                departed(src.at[part], send_sem.at[t, d])


def rows_out_body(n, root, src, ids, hot_src, hot_ids, table, table_out, rows, hot_rows, acc, pick, send_sem, recv_sem, own_sem, load_sem, hot_send, hot_recv, hot_own):
    me = lax.axis_index("dp")
    core = lax.rem(me, 2)
    is_root = me // 2 == root
    slices, _, size, width = hot_src.shape
    block, depth = pick.shape
    wide = 256
    blocks = acc.shape[0] // block
    mine = pl.ds(pl.multiple_of(me * size, size), size)
    others = pl.ds(0, (n - 1) * size)

    def own(k):
        return pltpu.make_async_copy(hot_src.at[k, core], hot_rows.at[k, mine], hot_own.at[k])

    def hot_to(k, to, dev):
        copy_to(hot_src.at[k, to], hot_rows.at[k, mine], hot_send, hot_recv.at[k], dev).start()

    def add(ids, rows):
        def one(i, carry):
            start = pl.multiple_of(lax.rem(i, blocks) * block, block)
            deep = pl.ds(pl.multiple_of(i // blocks * depth, depth), depth)
            row = lax.broadcasted_iota(jnp.int32, (block, depth), 0) + start
            pick[...] = (row == ids[:, deep]).astype(jnp.float32).astype(jnp.bfloat16)

            def columns(w, carry):
                part = pl.ds(pl.multiple_of(w * wide, wide), wide)
                acc[pl.ds(start, block), part] += jnp.dot(pick[...], rows[deep, part], preferred_element_type=jnp.float32)
                return carry

            return lax.fori_loop(0, width // wide, columns, carry)

        lax.fori_loop(0, blocks * (n * size // depth), one, None)

    def take(k, carry):
        arrived(hot_rows.at[k, others], hot_recv.at[k])
        own(k).wait()
        add(hot_ids.at[k], hot_rows.at[k])
        return carry

    def take_all(start, stop):
        if root < n // 2:
            @pl.when(is_root)
            def _():
                lax.fori_loop(start, stop, take, None)

    each_other(n, me, greet)
    load = pltpu.make_async_copy(table, acc, load_sem)
    load.start()
    pl.semaphore_wait(greet(), n - 1)
    if root < n // 2:
        @pl.when(is_root)
        def _():
            for k in range(slices):
                hot_to(k, 1 - core, me + 1 - 2 * core)
                own(k).start()

        @pl.when(jnp.logical_not(is_root))
        def _():
            for k in range(slices):
                for to in range(2):
                    hot_to(k, to, 2 * root + to)

    cold_own = pltpu.make_async_copy(src.at[me], rows.at[mine], own_sem)
    cold_own.start()
    each_other(n, me, lambda dev: copy_to(src.at[dev], rows.at[mine], send_sem, recv_sem, dev).start())
    load.wait()
    take_all(0, slices // 2)
    arrived(rows.at[others], recv_sem)
    cold_own.wait()
    add(ids, rows)
    take_all(slices // 2, slices)
    store = pltpu.make_async_copy(acc, table_out, load_sem)
    store.start()
    departed(rows.at[others], send_sem)
    if root < n // 2:
        @pl.when(is_root)
        def _():
            departed(hot_src.at[:, 0], hot_send)

        @pl.when(jnp.logical_not(is_root))
        def _():
            departed(hot_src, hot_send)

    store.wait()


def rows_out(n, root, src, ids, hot_src, hot_ids, table, collective_id):
    slices, _, size, width = hot_src.shape
    dma, vmem = pltpu.SemaphoreType.DMA, pl.BlockSpec(memory_space=pltpu.VMEM)
    shapes = ((n * size, width), (slices, n * size, width), table.shape, (1024, 512))
    return pl.pallas_call(
        functools.partial(rows_out_body, n, root),
        out_shape=jax.ShapeDtypeStruct(table.shape, table.dtype),
        in_specs=[ANY, vmem, ANY, vmem, ANY],
        out_specs=ANY,
        input_output_aliases={4: 0},
        scratch_shapes=[pltpu.VMEM(shape, table.dtype if shape == table.shape else src.dtype) for shape in shapes] + [dma] * 5 + [dma((slices,))] * 2,
        compiler_params=pltpu.CompilerParams(collective_id=collective_id, has_side_effects=True, vmem_limit_bytes=40 << 20),
        cost_estimate=pl.CostEstimate(flops=150 * 30_000_000, bytes_accessed=0, transcendentals=0),
        name=f"rows_out_{root}",
    )(src, ids, hot_src, hot_ids, table)


CAND_PARTS = ((0, 24, (3, 2, 1, 0)), (24, 24, (2, 3, 1, 0)), (48, 8, (1, 3, 2, 0)), (56, 8, (1, 2, 3, 0)))


def cand_sum_body(n, src, out, *refs):
    num = len(CAND_PARTS)
    acc, refs = refs[:num], refs[num:]
    got, (load_sem, recv_sem, send_sem) = [refs[i * num:(i + 1) * num] for i in range(5)], refs[5 * num:]
    me = lax.axis_index("dp")
    core = lax.rem(me, 2)
    bit = [lax.rem(me // d, 2) for d in (16, 8, 4, 2)]
    across = [me + d * (1 - 2 * b) for d, b in zip((16, 8, 4, 2), bit)]
    partner = me + 1 - 2 * core
    every = slice(None)

    pl.semaphore_wait(greet(partner, *across), 5)

    for p, (at, rows, _) in enumerate(CAND_PARTS):
        w = pl.ds(at, rows)
        copy_to(src.at[:, :, :, :, 1 - core, w], got[0][p], send_sem.at[0, p], recv_sem.at[0, p], partner).start()
        pltpu.make_async_copy(src.at[:, :, :, :, core, w], acc[p], load_sem.at[p]).start()

    def add(p, level, fixed):
        held = CAND_PARTS[p][2][:level]
        free = [a for a in range(4) if fixed[a] is every]
        for k in range(2 ** len(free)):
            index = list(fixed)
            for j, a in enumerate(free):
                index[a] = k >> j & 1
            there = tuple(index[a] for a in range(4) if a not in held)
            acc[p][tuple(index)] += got[level][p][there]

    for level in range(5):
        for p, (at, rows, dims) in enumerate(CAND_PARTS):
            if level == 0:
                pltpu.make_async_copy(acc[p], acc[p], load_sem.at[p]).wait()
            arrived(got[level][p], recv_sem.at[level, p])
            fixed = [bit[a] if a in dims[:level] else every for a in range(4)]
            if level == 4:
                out[pl.ds(at, rows)] = acc[p][tuple(fixed)] + got[4][p][...]
                continue
            axis = dims[level]
            away, kept = list(fixed), list(fixed)
            away[axis], kept[axis] = 1 - bit[axis], bit[axis]
            add(p, level, away)
            copy_to(acc[p].at[tuple(away)], got[level + 1][p], send_sem.at[level + 1, p], recv_sem.at[level + 1, p], across[axis]).start()
            add(p, level, kept)
    for level in range(5):
        for p in range(num):
            departed(got[level][p], send_sem.at[level, p])


def cand_sum(n, part, collective_id):
    width = part.shape[1]
    dma = pltpu.SemaphoreType.DMA
    sizes = [[(2,) * (4 - level) + (rows, width) for _, rows, _ in CAND_PARTS] for level in range(5)]
    return pl.pallas_call(
        functools.partial(cand_sum_body, n),
        out_shape=jax.ShapeDtypeStruct((part.shape[0] // n, width), part.dtype),
        in_specs=[ANY],
        out_specs=pl.BlockSpec(memory_space=pltpu.VMEM),
        scratch_shapes=[pltpu.VMEM(s, part.dtype) for level in [0] + list(range(5)) for s in sizes[level]] + [dma((len(CAND_PARTS),)), dma((5, len(CAND_PARTS))), dma((5, len(CAND_PARTS)))],
        compiler_params=pltpu.CompilerParams(collective_id=collective_id, has_side_effects=True, vmem_limit_bytes=20 << 20),
        cost_estimate=pl.CostEstimate(flops=40 * 30_000_000, bytes_accessed=0, transcendentals=0),
        name="cand_sums",
    )(part.reshape(2, 2, 2, 2, 2, part.shape[0] // n, width))


X, Y, Z1, Z2 = 2, 4, 8, 16
PARTS = ((0, 512, (X, Y, Z1, Z2)), (512, 256, (Z1, X, Y, Z2)), (768, 512, (Y, X, Z1, Z2)), (1280, 256, (Z1, Y, X, Z2)))
GROUP = 1536


def sum_body(n, groups, srcs, note, outs, note_out, acc, got, notes, load_sem, pair_sem, half_sem, full_sem, send_sem, out_sem, note_sem):
    me = lax.axis_index("dp")
    core = lax.rem(me, 2)
    partner = me + 1 - 2 * core
    bit = {d: lax.rem(me // d, 2) for d in (X, Y, Z1, Z2)}
    across = {d: me + d * (1 - 2 * bit[d]) for d in bit}
    per_src = groups // len(srcs)
    full = got[0]
    width = acc.shape[-1]

    def area(ref, group, start, shift, size):
        high = ref.shape[0]
        if ref.shape[1] == width:
            return ref.at[pl.ds(pl.multiple_of(group * GROUP + start + shift, 8), size)]
        column = pl.multiple_of((group * (GROUP // high) + start // high) * width, width)
        return ref.at[pl.ds(pl.multiple_of(start % high + shift, 8), size), pl.ds(column, width)]

    def spot(part, level):
        start, rows, dims = part
        at, size = start // 2, rows // 2
        for d in dims[:level]:
            size //= 2
            at = at + bit[d] * size
        return at if level == 0 else pl.multiple_of(at, 8), size

    def away(part, level):
        at, size = spot(part, level)
        return pl.multiple_of(at + (1 - bit[part[2][level]]) * (size // 2), 8), size // 2

    each_other(n, me, greet)
    for g in range(groups):
        for start, rows, _ in PARTS:
            half = rows // 2
            mine = area(srcs[g // per_src], g % per_src, start, core * half, half)
            pltpu.make_async_copy(mine, acc.at[g, pl.ds(start // 2, half)], load_sem.at[g]).start()
    notes[me] = note[...]
    pl.semaphore_wait(greet(), n - 1)

    for g in range(groups):
        for start, rows, _ in PARTS:
            half = rows // 2
            other = area(srcs[g // per_src], g % per_src, start, (1 - core) * half, half)
            copy_to(other, full.at[g, pl.ds(start // 2, half)], send_sem.at[0], pair_sem.at[g], partner).start()

    each_other(n, me, lambda dev: copy_to(note, notes.at[me], note_sem.at[0], note_sem.at[1], dev).start())

    def add(dst, at, x, x_at, y, y_at, size, g):
        block = min(size, 32)

        def one(i, carry):
            k = pl.multiple_of(i * block, block)
            dst[g, pl.ds(at + k, block)] = x[g, pl.ds(x_at + k, block)] + y[g, pl.ds(y_at + k, block)]
            return carry

        lax.fori_loop(0, size // block, one, None)

    def advance(stage, g):
        if stage == 0:
            pltpu.make_async_copy(acc.at[g], acc.at[g], load_sem.at[g]).wait()
            arrived(full.at[g], pair_sem.at[g])
        for p, part in enumerate(PARTS):
            start, rows, dims = part
            if stage <= 4:
                at, size = spot(part, stage)
                in_at = start >> (stage + 1)
                if stage:
                    arrived(got[stage].at[g, pl.ds(in_at, size)], half_sem.at[stage - 1, p, g])
                if stage < 4:
                    add(acc, at, acc, at, got[stage], in_at, size, g)
                    off, half = away(part, stage)
                    copy_to(acc.at[g, pl.ds(off, half)], got[stage + 1].at[g, pl.ds(start >> (stage + 2), half)],
                            send_sem.at[stage + 1], half_sem.at[stage, p, g], across[dims[stage]]).start()
                    continue
                add(full, at, acc, at, got[stage], in_at, size, g)
            else:
                back_at, back = spot(part, 9 - stage)
                there = full.at[g, pl.ds(pl.multiple_of(back_at + (1 - 2 * bit[dims[8 - stage]]) * back, 8), back)]
                arrived(there, full_sem.at[stage - 5, p, g])
                at, size = spot(part, 8 - stage)
            if stage < 8:
                held = full.at[g, pl.ds(at, size)]
                copy_to(held, held, send_sem.at[stage + 1], full_sem.at[stage - 4, p, g], across[dims[7 - stage]]).start()
            else:
                half = rows // 2
                held = full.at[g, pl.ds(start // 2, half)]
                for i, out in enumerate(outs):
                    @pl.when(g // per_src == i)
                    def _():
                        place = area(out, lax.rem(g, per_src), start, core * half, half)
                        copy_to(held, place, send_sem.at[9], out_sem.at[0], partner).start()
                        pltpu.make_async_copy(held, place, out_sem.at[1]).start()

    def tick(k, carry):
        for stage in reversed(range(9)):
            g = k - stage
            pl.when((g >= 0) & (g < groups))(functools.partial(advance, stage, g))
        return carry

    lax.fori_loop(0, groups + 8, tick, None)

    departed(notes.at[pl.ds(0, n - 1)], note_sem.at[0])
    arrived(notes.at[pl.ds(0, n - 1)], note_sem.at[1])
    note_out[...] = jnp.sum(notes[...], axis=0)
    for i, sent in enumerate(got):
        departed(sent, send_sem.at[i])
        departed(sent, send_sem.at[9 - i])
    arrived(full, out_sem.at[0])
    pltpu.make_async_copy(full, full, out_sem.at[1]).wait()


def sum_over_devices(n, srcs, note, collective_id):
    width = min(srcs[0].shape)
    groups = len(srcs) * srcs[0].size // (GROUP * width)
    sizes = [(groups, GROUP // 2 >> i, width) for i in range(5)]

    def body(*refs):
        rest = iter(refs)
        ins, note_in = [next(rest) for _ in srcs], next(rest)
        outs, note_out = [next(rest) for _ in srcs], next(rest)
        acc, got = next(rest), [next(rest) for _ in sizes]
        sum_body(n, groups, ins, note_in, outs, note_out, acc, got, *rest)

    vmem = pl.BlockSpec(memory_space=pltpu.VMEM)
    dma = pltpu.SemaphoreType.DMA
    return pl.pallas_call(
        body,
        out_shape=tuple(jax.ShapeDtypeStruct(x.shape, jnp.float32) for x in tuple(srcs) + (note,)),
        in_specs=[ANY] * len(srcs) + [vmem],
        out_specs=(ANY,) * len(srcs) + (vmem,),
        scratch_shapes=[pltpu.VMEM(sizes[0], jnp.float32)] + [pltpu.VMEM(s, jnp.float32) for s in sizes] + [
            pltpu.VMEM((n,) + note.shape, jnp.float32),
            dma((groups,)), dma((groups,)), dma((4, len(PARTS), groups)), dma((4, len(PARTS), groups)), dma((10,)), dma((2,)), dma((2,)),
        ],
        compiler_params=pltpu.CompilerParams(collective_id=collective_id, has_side_effects=True, vmem_limit_bytes=32 << 20),
        cost_estimate=pl.CostEstimate(flops=200 * 30_000_000, bytes_accessed=0, transcendentals=0),
        name="weight_sums",
    )(*srcs, note)


def comm_call(body, srcs, out_shapes, collective_id, name, sems=((), (), ())):
    return pl.pallas_call(
        body,
        out_shape=[jax.ShapeDtypeStruct(shape, srcs[0].dtype) for shape in out_shapes],
        in_specs=[ANY] * len(srcs),
        out_specs=[ANY] * len(out_shapes),
        scratch_shapes=[pltpu.SemaphoreType.DMA(shape) if shape else pltpu.SemaphoreType.DMA for shape in sems],
        compiler_params=pltpu.CompilerParams(collective_id=collective_id, has_side_effects=True),
        cost_estimate=pl.CostEstimate(flops=50 * 30_000_000, bytes_accessed=0, transcendentals=0),
        name=name,
    )(*srcs)


def solution(mesh):
    n = mesh.shape["dp"]

    def local_step(tokens, w_one, w_two, wi_one, wi_two, table_loc, cand_ids, log_q, targ_loc):
        me = lax.axis_index("dp")
        rows_loc, width = table_loc.shape
        num_tok = tokens.shape[0]
        num_cand = cand_ids.shape[0]
        cand_loc = num_cand // n
        num_req = num_tok + cand_loc
        tok_total = num_tok * n

        def swap(src, collective_id, name):
            return comm_call(functools.partial(all_to_all_body, n), [src], [src.shape], collective_id, name)[0]

        cand_at = cand_ids - me * rows_loc
        cand_here = (cand_at >= 0) & (cand_at < rows_loc)
        cand_rows = jnp.where(cand_here[:, None], jnp.take(table_loc, jnp.clip(cand_at, 0, rows_loc - 1), axis=0), 0)
        cand_mine = lax.psum_scatter(cand_rows, "dp", scatter_dimension=0, tiled=True)
        cand_vec_mine = tower_fwd(cand_mine, wi_one, wi_two)[2]

        req_ids = jnp.concatenate([targ_loc, lax.dynamic_slice(cand_ids, (me * cand_loc,), (cand_loc,))])
        owner = req_ids // rows_loc
        local_id = req_ids - owner * rows_loc
        is_owner = (owner[:, None] == jnp.arange(n)[None, :]).astype(jnp.bfloat16)
        earlier = (jnp.arange(num_req)[:, None] > jnp.arange(num_req)[None, :]).astype(jnp.bfloat16)
        before = jnp.dot(earlier, is_owner, preferred_element_type=jnp.float32)
        is_owner_f = is_owner.astype(jnp.float32)
        rank = jnp.sum(before * is_owner_f, axis=1).astype(jnp.int32)
        counts = jnp.sum(is_owner_f, axis=0).astype(jnp.int32)

        depth = -(-num_req // 128) * 128
        is_rank = (rank[:, None] == jnp.arange(depth)[None, :]).astype(jnp.bfloat16)
        place = jnp.arange(num_req)
        halves = [local_id // 64, local_id % 64, place // 64, place % 64, jnp.ones_like(place)]
        picks = jnp.concatenate([is_owner * h.astype(jnp.bfloat16)[:, None] for h in halves], axis=1)
        tables = jnp.einsum("ia,ij->aj", picks, is_rank, preferred_element_type=jnp.float32).astype(jnp.int32).reshape(5, n, depth)
        want_ids = jnp.where(tables[4] > 0, tables[0] * 64 + tables[1], -1)
        places = tables[2] * 64 + tables[3]

        lines = depth // 128
        note = jnp.concatenate([
            want_ids.reshape(n, lines, 128),
            jnp.broadcast_to(jnp.pad(counts, (0, 128 - n))[None, None, :], (n, 16 - lines, 128)),
        ], axis=1)
        notes = swap(note, 0, "notes")
        ask_ids = notes[:, :lines].reshape(n, depth)
        all_counts = notes[:, lines, :n]

        most = jnp.max(all_counts)
        too_many = most > PAIR_ROWS + HOT_ROWS
        extra_rounds = jnp.where(too_many, (most + PAIR_ROWS - 1) // PAIR_ROWS - 1, 0)
        hot_chip = jnp.max(all_counts.reshape(n, n // 2, 2), axis=(0, 2)) > PAIR_ROWS
        num_hot = jnp.sum(hot_chip.astype(jnp.int32))
        hot_rank = jnp.sum((jnp.arange(n // 2)[None, :] < jnp.arange(n // 2)[:, None]) & hot_chip[None, :], axis=1)

        def hot_at(i):
            return jnp.sum(jnp.where(hot_chip & (hot_rank == i), jnp.arange(n // 2), 0))

        ask_pad = jnp.pad(ask_ids, ((0, 0), (0, HOT_ROWS)), constant_values=-1)
        place_pad = jnp.pad(places, ((0, 0), (0, HOT_ROWS)))

        def window(table, at, size):
            return lax.dynamic_slice(table, (0, at), (table.shape[0], size))

        def fetch(ids):
            picked = jnp.take(table_loc, jnp.maximum(ids.reshape(-1), 0), axis=0)
            return picked.reshape(ids.shape + (width,))

        rows_out_src = fetch(ask_ids[:, :PAIR_ROWS])
        none = n // 2

        def come_in(i, carry):
            rows = carry[0]
            chip = jnp.where(i < num_hot, hot_at(i), none)

            def from_root(root):
                sems = ((), (), (), (3, 4), (3, -(-CHUNKS // 3)), (), (), (), ())
                return lambda src, table: comm_call(functools.partial(rows_in_body, n, root), [src, table], [src.shape, (2, rows_loc, width)], 4 + root, f"rows_in_{root}", sems)

            got, blocks = lax.switch(chip, [from_root(k) for k in range(none + 1)], rows_out_src, table_loc)
            found = jnp.take(blocks.reshape(-1, width), lax.rem(owner, 2) * rows_loc + local_id, axis=0)
            return jnp.where((owner // 2 == chip)[:, None], found, rows), got

        hot_raw, got = lax.fori_loop(0, jnp.maximum(num_hot, 1), come_in, (jnp.zeros((num_req, width), jnp.bfloat16), jnp.zeros_like(rows_out_src)))
        got, cand_vec_mine = lax.optimization_barrier((got, cand_vec_mine))
        cand_vec = lax.all_gather(cand_vec_mine, "dp", axis=0, tiled=True)
        slot = owner * PAIR_ROWS + jnp.clip(rank, 0, PAIR_ROWS - 1)
        from_hot = jnp.any((owner[:, None] // 2 == jnp.arange(n // 2)[None, :]) & hot_chip[None, :], axis=1)
        raw = jnp.where(from_hot[:, None], hot_raw, jnp.take(got.reshape(-1, width), slot, axis=0))

        i_pre, i_hidden, i_vec = tower_fwd(raw, wi_one, wi_two)
        targ_vec = i_vec[:num_tok]
        q_pre, q_hidden, query = tower_fwd(tokens, w_one, w_two)
        loss_sum, d_query, d_targ_vec, dz_cand, logit_scale = loss_grads(query, targ_vec, cand_vec, log_q, targ_loc, cand_ids, tok_total)
        d_cand_part = jnp.einsum("ts,td->sd", dz_cand, query, preferred_element_type=jnp.float32)
        dw_one, dw_two = tower_back(tokens, w_two, q_pre, q_hidden, d_query)[1:]
        d_cand_part, dw_one, dw_two = lax.optimization_barrier((d_cand_part, dw_one, dw_two))
        query_sums = lax.psum((dw_one, dw_two), "dp")
        d_cand_vec = (cand_sum(n, d_cand_part, 3) * logit_scale).astype(jnp.bfloat16)
        d_vec = jnp.concatenate([d_targ_vec, d_cand_vec])
        i_grad_pre, dwi_one, dwi_two = tower_back(raw, wi_two, i_pre, i_hidden, d_vec)
        d_raw = jnp.einsum("nf,df->nd", i_grad_pre, wi_one, preferred_element_type=jnp.float32).astype(jnp.bfloat16)
        def spread(ids):
            return jnp.take(d_raw, ids.reshape(-1), axis=0).reshape(ids.shape + (width,))

        def add_rows(acc, ids, rows):
            ids = ids.reshape(-1)
            ids = jnp.where(ids >= 0, ids, rows_loc)
            return acc.at[ids].add(rows.reshape(-1, width).astype(jnp.float32), mode="drop")

        cold_src = spread(places[:, :PAIR_ROWS])
        cold_ids = ask_ids[:, :PAIR_ROWS].reshape(1, n * PAIR_ROWS)
        hot_ids = ask_ids[:, PAIR_ROWS:PAIR_ROWS + HOT_ROWS].reshape(n, SLICES, HOT_ROWS // SLICES)
        hot_ids = hot_ids.transpose(1, 0, 2).reshape(SLICES, 1, n * HOT_ROWS // SLICES)
        hot_back = jnp.where(too_many, 0, num_hot)

        def go_out(i, acc):
            chip = jnp.where(i < hot_back, hot_at(i), none)
            hot_places = lax.dynamic_slice(places, (2 * jnp.minimum(chip, none - 1), PAIR_ROWS), (2, HOT_ROWS))
            hot_places = hot_places.reshape(2, SLICES, HOT_ROWS // SLICES).transpose(1, 0, 2)

            def to_root(root):
                return lambda *args: rows_out(n, root, *args, 4 + n + root)

            return lax.switch(chip, [to_root(k) for k in range(none + 1)], cold_src, jnp.where(i > 0, -1, cold_ids), spread(hot_places), hot_ids, acc)

        d_table = lax.fori_loop(0, jnp.maximum(hot_back, 1), go_out, jnp.zeros((rows_loc, width), jnp.float32))

        def extra_out(r, acc):
            back = swap(spread(window(place_pad, r * PAIR_ROWS, PAIR_ROWS)), 1, "rows_more")
            return add_rows(acc, window(ask_pad, r * PAIR_ROWS, PAIR_ROWS), back)

        d_table = lax.fori_loop(1, 1 + extra_rounds, extra_out, d_table)
        loss_note, d_table = lax.optimization_barrier((jnp.full((8, 128), loss_sum, jnp.float32), d_table))
        dwi_one, dwi_two, loss_note = sum_over_devices(n, (dwi_one, dwi_two), loss_note, 2)
        loss = loss_note[0, 0] / tok_total
        return loss, d_table, query_sums[0], query_sums[1], dwi_one, dwi_two

    return jax.shard_map(local_step, mesh=mesh, in_specs=(P("dp", None), P(), P(), P(), P(), P("dp", None), P(), P(), P("dp")), out_specs=(P(), P("dp", None), P(), P(), P(), P()), check_vma=False)
```

```python
import functools
import math
import jax
import jax.numpy as jnp
from jax import lax
from jax.experimental import pallas as pl
from jax.experimental.pallas import tpu as pltpu
from jax.sharding import PartitionSpec as P

SCORE_GAIN = 3.0
HIT_VALUE = -1e9
PAIR_ROWS = 48
SLICES = 5
HOT_ROWS = SLICES * PAIR_ROWS
CHUNKS = 128
LAG = 3
MESH = pl.DeviceIdType.MESH
ANY = pl.BlockSpec(memory_space=pl.ANY)


def tower_fwd(row_block, w_in, w_out):
    pre_act = jnp.dot(row_block, w_in, preferred_element_type=jnp.float32)
    hidden = jax.nn.gelu(pre_act).astype(jnp.bfloat16)
    tower_out = jnp.dot(hidden, w_out, preferred_element_type=jnp.float32).astype(jnp.bfloat16)
    return pre_act, hidden, tower_out


def tower_back(row_block, w_out, pre_act, hidden, grad_out):
    dw_out = jnp.einsum("nf,nd->fd", hidden, grad_out, preferred_element_type=jnp.float32)
    grad_hidden = jnp.einsum("nd,fd->nf", grad_out, w_out, preferred_element_type=jnp.float32)
    gelu_back = jax.vjp(jax.nn.gelu, pre_act)[1]
    grad_pre = gelu_back(grad_hidden)[0].astype(jnp.bfloat16)
    dw_in = jnp.einsum("ne,nf->ef", row_block, grad_pre, preferred_element_type=jnp.float32)
    return grad_pre, dw_in, dw_out


def loss_grads(query, targ_vec, cand_vec, log_q, targ_ids, cand_ids, tok_total):
    logit_scale = SCORE_GAIN / math.sqrt(query.shape[1])
    z_targ = jnp.einsum("td,td->t", query, targ_vec, preferred_element_type=jnp.float32) * logit_scale
    z_cand = jnp.einsum("td,sd->ts", query, cand_vec, preferred_element_type=jnp.float32) * logit_scale - log_q[None, :]
    z_cand = jnp.where(targ_ids[:, None] == cand_ids[None, :], HIT_VALUE, z_cand)
    row_max = jnp.maximum(z_targ, jnp.max(z_cand, axis=1))
    e_targ = jnp.exp(z_targ - row_max)
    e_cand = jnp.exp(z_cand - row_max[:, None])
    denom_sum = e_targ + jnp.sum(e_cand, axis=1)
    loss_sum = jnp.sum(jnp.log(denom_sum) + row_max - z_targ)
    dz_targ = ((e_targ / denom_sum - 1.0) / tok_total).astype(jnp.bfloat16).astype(jnp.float32)
    dz_cand = (e_cand / denom_sum[:, None] / tok_total).astype(jnp.bfloat16)
    d_query = ((dz_targ[:, None] * targ_vec.astype(jnp.float32) + jnp.einsum("ts,sd->td", dz_cand, cand_vec, preferred_element_type=jnp.float32)) * logit_scale).astype(jnp.bfloat16)
    d_targ_vec = (logit_scale * dz_targ[:, None] * query.astype(jnp.float32)).astype(jnp.bfloat16)
    return loss_sum, d_query, d_targ_vec, dz_cand, logit_scale


def how(collective_id, us):
    return dict(
        compiler_params=pltpu.CompilerParams(collective_id=collective_id, has_side_effects=True, vmem_limit_bytes=34 << 20),
        cost_estimate=pl.CostEstimate(flops=us * 30_000_000, bytes_accessed=0, transcendentals=0),
    )


def copy_to(src, dst, send_sem, recv_sem, dev):
    return pltpu.make_async_remote_copy(src, dst, send_sem, recv_sem, device_id=(dev,), device_id_type=MESH)


def greet(*devs):
    barrier = pltpu.get_barrier_semaphore()
    for dev in devs:
        pl.semaphore_signal(barrier, device_id=(dev,), device_id_type=MESH)
    return barrier


def each_other(n, me, act):
    def one(i, carry):
        act(lax.rem(me + i, n))
        return carry

    lax.fori_loop(1, n, one, None)


def arrived(ref, sem):
    copy_to(ref, ref, sem, sem, lax.axis_index("dp")).wait_recv()


def departed(ref, sem):
    copy_to(ref, ref, sem, sem, lax.axis_index("dp")).wait_send()


def swap_start(n, me, src, place, send_sem, recv_sem, own_sem):
    pltpu.make_async_copy(src.at[me], place(me), own_sem).start()
    each_other(n, me, lambda dev: copy_to(src.at[dev], place(me), send_sem, recv_sem, dev).start())


def swap_end(n, me, src, send_sem, recv_sem, own_sem):
    pltpu.make_async_copy(src.at[me], src.at[me], own_sem).wait()
    departed(src.at[pl.ds(0, n - 1)], send_sem)
    arrived(src.at[pl.ds(0, n - 1)], recv_sem)


def all_to_all_body(n, src, dst, *sems):
    me = lax.axis_index("dp")
    each_other(n, me, greet)
    pl.semaphore_wait(greet(), n - 1)
    swap_start(n, me, src, lambda s: dst.at[s], *sems)
    swap_end(n, me, src, *sems)


TREES = (
    ((4368, 13104, 273, 224), (17476, 52425, 1092, 0), (43689, 2, 2730, 0)),
    ((4353, 13059, 284, 528), (17476, 52380, 1088, 64), (43674, 32, 2720, 160)),
)


def tree_depths(masks, start, chips):
    depth = {start: 0}
    while len(depth) < chips:
        for c, at in tuple(depth.items()):
            for d, to in enumerate((c ^ 1, c ^ 2, c + 4, c - 4)):
                if masks[d] >> c & 1:
                    depth[to] = at + 1
    return depth


def rows_in_body(n, root, src, table, dst, send_sem, recv_sem, own_sem, *sems):
    me = lax.axis_index("dp")
    high, size = table.shape[0], src.shape[1]
    each_other(n, me, greet)
    pl.semaphore_wait(greet(), n - 1)
    swap_start(n, me, src, lambda s: dst.at[pl.ds(pl.multiple_of(2 * high + s * size, 16), size)], send_sem, recv_sem, own_sem)
    if root < n // 2:
        broadcast(n, root, table, lambda core: dst.at[pl.ds(pl.multiple_of(core * high, high), high)], *sems)
    swap_end(n, me, src, send_sem, recv_sem, own_sem)


def broadcast(n, root, src, dst, send_sem, recv_sem, pair_send, pair_recv, echo_send, echo_recv):
    me = lax.axis_index("dp")
    core = lax.rem(me, 2)
    chip = me // 2
    at_x, at_y, at_z = lax.rem(chip, 2), lax.rem(chip // 2, 2), chip // 4
    root_z = root // 4
    up = 1 if root_z < 2 else -1
    rel_z = at_z if root_z < 2 else 3 - at_z
    rel = (rel_z * 2 + lax.rem(at_y + root // 2, 2)) * 2 + lax.rem(at_x + root, 2)
    is_root = chip == root
    trees = TREES[min(root_z, 3 - root_z)]
    to = (me + 2 - 4 * at_x, me + 4 - 8 * at_y, me + 8 * up, me - 8 * up)
    partner = me + 1 - 2 * core

    def passes(mask):
        hit = rel < 0
        for c in range(n // 2):
            if mask >> c & 1:
                hit = hit | (rel == c)
        return hit

    moves = [[(d, passes(trees[t][d])) for d in range(4) if trees[t][d]] for t in range(3)]
    depths = [tree_depths(trees[t], 4 * min(root_z, 3 - root_z), n // 2) for t in range(3)]
    behind = [LAG * sum((rel == c).astype(jnp.int32) * depths[t][c] for c in range(n // 2)) for t in range(3)]

    rows = src.shape[0] // CHUNKS
    steps = -(-CHUNKS // 3)

    def step(held, j, t):
        piece = pl.ds((3 * j + t) * rows, rows)
        for d, on in moves[t]:
            @pl.when(on)
            def _():
                copy_to(held.at[piece], dst(core).at[piece], send_sem.at[t, d], recv_sem.at[t, j], to[d]).start()

    @pl.when(is_root)
    def _():
        copy_to(src, dst(core), pair_send, pair_recv, partner).start()

        def go(j, carry):
            for t in range(3):
                pl.when(3 * j + t < CHUNKS)(functools.partial(step, src, j, t))
            return carry

        lax.fori_loop(0, steps, go, None)
        arrived(dst(1 - core), pair_recv)
        copy_to(dst(1 - core), dst(1 - core), echo_send, echo_recv, partner).start()
        copy_to(dst(core), dst(core), echo_send, echo_recv, partner).wait()

    @pl.when(jnp.logical_not(is_root))
    def _():
        held = dst(core)

        def relay(t, j):
            piece = pl.ds((3 * j + t) * rows, rows)
            arrived(held.at[piece], recv_sem.at[t, j])
            step(held, j, t)
            copy_to(held.at[piece], dst(core).at[piece], pair_send, pair_recv, partner).start()

        def go(i, carry):
            for t in range(3):
                j = i - behind[t]
                pl.when((j >= 0) & (3 * j + t < CHUNKS))(functools.partial(relay, t, j))
            return carry

        far = max(max(d.values()) for d in depths)
        lax.fori_loop(LAG, steps + LAG * far, go, None)
        arrived(held, pair_recv)

    departed(src, pair_send)
    for t in range(3):
        part = pl.ds(0, len(range(t, CHUNKS, 3)) * rows)
        for d, on in moves[t]:
            @pl.when(on)
            def _():
                departed(src.at[part], send_sem.at[t, d])


def rows_out_body(n, root, src, hot_src, ids, table, table_out, rows, relay, acc, pick, send_sem, recv_sem, own_sem, relay_sem, load_sem):
    me = lax.axis_index("dp")
    core, chip = lax.rem(me, 2), me // 2
    is_root = chip == root
    slices, _, size, width = hot_src.shape
    block, depth = pick.shape
    wide = 256
    blocks = acc.shape[0] // block
    others = pl.ds(0, (n - 1) * size)

    def place(s):
        return pl.ds(pl.multiple_of(s * size, size), size)

    def take(k):
        arrived(rows.at[k, others], recv_sem.at[k])
        pltpu.make_async_copy(src.at[me], rows.at[k, place(me)], own_sem.at[k]).wait()

        def add(i, carry):
            start = pl.multiple_of(lax.rem(i, blocks) * block, block)
            deep = pl.ds(pl.multiple_of(i // blocks * depth, depth), depth)
            row = lax.broadcasted_iota(jnp.int32, (block, depth), 0) + start
            pick[...] = (row == ids[k, :, deep]).astype(jnp.float32).astype(jnp.bfloat16)

            def columns(w, carry):
                part = pl.ds(pl.multiple_of(w * wide, wide), wide)
                acc[pl.ds(start, block), part] += jnp.dot(pick[...], rows[k, deep, part], preferred_element_type=jnp.float32)
                return carry

            return lax.fori_loop(0, width // wide, columns, carry)

        lax.fori_loop(0, blocks * (n * size // depth), add, None)

    each_other(n, me, greet)
    load = pltpu.make_async_copy(table, acc, load_sem)
    load.start()
    pl.semaphore_wait(greet(), n - 1)
    pltpu.make_async_copy(src.at[me], rows.at[0, place(me)], own_sem.at[0]).start()
    each_other(n, me, lambda dev: copy_to(src.at[dev], rows.at[0, place(me)], send_sem.at[0], recv_sem.at[0], dev).start())
    if root < n // 2:
        off_x, off_y = lax.rem(chip + root, 2), lax.rem(chip // 2 + root // 2, 2)
        aside = me + 2 - 4 * lax.rem(chip, 2)
        on_turn = (off_y == 1) & (lax.rem(me // 8, 2) == 1)
        goes_aside, relays = on_turn & (off_x == 1), on_turn & (off_x == 0)

        @pl.when(is_root)
        def _():
            for k in range(slices):
                copy_to(hot_src.at[k, 1 - core], rows.at[k + 1, place(me)], send_sem.at[1], recv_sem.at[k + 1], me + 1 - 2 * core).start()
                pltpu.make_async_copy(hot_src.at[k, core], rows.at[k + 1, place(me)], own_sem.at[k + 1]).start()

        @pl.when(goes_aside)
        def _():
            for k in range(slices):
                copy_to(hot_src.at[k], relay.at[k], send_sem.at[1], relay_sem.at[k], aside).start()

        @pl.when(jnp.logical_not(is_root | goes_aside))
        def _():
            for k in range(slices):
                for to in range(2):
                    copy_to(hot_src.at[k, to], rows.at[k + 1, place(me)], send_sem.at[1], recv_sem.at[k + 1], 2 * root + to).start()

        @pl.when(relays)
        def _():
            for k in range(slices):
                arrived(relay.at[k], relay_sem.at[k])
                for to in range(2):
                    copy_to(relay.at[k, to], rows.at[k + 1, place(aside)], send_sem.at[2], recv_sem.at[k + 1], 2 * root + to).start()

    load.wait()

    def take_if_mine(k, carry):
        pl.when((k == 0) | is_root)(functools.partial(take, k))
        return carry

    lax.fori_loop(0, slices + 1 if root < n // 2 else 1, take_if_mine, None)
    store = pltpu.make_async_copy(acc, table_out, load_sem)
    store.start()
    departed(rows.at[0, others], send_sem.at[0])
    if root < n // 2:
        @pl.when(is_root)
        def _():
            departed(hot_src.at[:, 0], send_sem.at[1])

        @pl.when(jnp.logical_not(is_root))
        def _():
            departed(hot_src, send_sem.at[1])

        @pl.when(relays)
        def _():
            departed(relay, send_sem.at[2])

    store.wait()


def rows_out(n, root, src, hot_src, ids, table, collective_id):
    slices, _, size, width = hot_src.shape
    dma = pltpu.SemaphoreType.DMA
    shapes = ((slices + 1, n * size, width), hot_src.shape, table.shape, (1024, 512))
    return pl.pallas_call(
        functools.partial(rows_out_body, n, root),
        out_shape=jax.ShapeDtypeStruct(table.shape, table.dtype),
        in_specs=[ANY, ANY, pl.BlockSpec(memory_space=pltpu.VMEM), ANY],
        out_specs=ANY,
        input_output_aliases={3: 0},
        scratch_shapes=[pltpu.VMEM(shape, table.dtype if shape == table.shape else src.dtype) for shape in shapes]
        + [dma((3,)), dma((slices + 1,)), dma((slices + 1,)), dma((slices,)), dma],
        **how(collective_id, 150),
        name=f"rows_out_{root}",
    )(src, hot_src, ids, table)


CAND_PARTS = ((0, 24, (3, 2, 1, 0)), (24, 24, (2, 3, 1, 0)), (48, 8, (1, 3, 2, 0)), (56, 8, (1, 2, 3, 0)))


def cand_sum_body(n, src, out, *refs):
    num = len(CAND_PARTS)
    acc, refs = refs[:num], refs[num:]
    got, (load_sem, recv_sem, send_sem) = [refs[i * num:(i + 1) * num] for i in range(5)], refs[5 * num:]
    me = lax.axis_index("dp")
    core = lax.rem(me, 2)
    bit = [lax.rem(me // d, 2) for d in (16, 8, 4, 2)]
    across = [me + d * (1 - 2 * b) for d, b in zip((16, 8, 4, 2), bit)]
    partner = me + 1 - 2 * core
    every = slice(None)

    pl.semaphore_wait(greet(partner, *across), 5)

    for p, (at, rows, _) in enumerate(CAND_PARTS):
        w = pl.ds(at, rows)
        copy_to(src.at[:, :, :, :, 1 - core, w], got[0][p], send_sem.at[0, p], recv_sem.at[0, p], partner).start()
        pltpu.make_async_copy(src.at[:, :, :, :, core, w], acc[p], load_sem.at[p]).start()

    def add(p, level, fixed):
        held = CAND_PARTS[p][2][:level]
        free = [a for a in range(4) if fixed[a] is every]
        for k in range(2 ** len(free)):
            index = list(fixed)
            for j, a in enumerate(free):
                index[a] = k >> j & 1
            there = tuple(index[a] for a in range(4) if a not in held)
            acc[p][tuple(index)] += got[level][p][there]

    for level in range(5):
        for p, (at, rows, dims) in enumerate(CAND_PARTS):
            if level == 0:
                pltpu.make_async_copy(acc[p], acc[p], load_sem.at[p]).wait()
            arrived(got[level][p], recv_sem.at[level, p])
            fixed = [bit[a] if a in dims[:level] else every for a in range(4)]
            if level == 4:
                out[pl.ds(at, rows)] = acc[p][tuple(fixed)] + got[4][p][...]
                continue
            axis = dims[level]
            away, kept = list(fixed), list(fixed)
            away[axis], kept[axis] = 1 - bit[axis], bit[axis]
            add(p, level, away)
            copy_to(acc[p].at[tuple(away)], got[level + 1][p], send_sem.at[level + 1, p], recv_sem.at[level + 1, p], across[axis]).start()
            add(p, level, kept)
    for level in range(5):
        for p in range(num):
            departed(got[level][p], send_sem.at[level, p])


def cand_sum(n, part, collective_id):
    width = part.shape[1]
    dma = pltpu.SemaphoreType.DMA
    sizes = [[(2,) * (4 - level) + (rows, width) for _, rows, _ in CAND_PARTS] for level in range(5)]
    return pl.pallas_call(
        functools.partial(cand_sum_body, n),
        out_shape=jax.ShapeDtypeStruct((part.shape[0] // n, width), part.dtype),
        in_specs=[ANY],
        out_specs=pl.BlockSpec(memory_space=pltpu.VMEM),
        scratch_shapes=[pltpu.VMEM(s, part.dtype) for level in [0] + list(range(5)) for s in sizes[level]] + [dma((len(CAND_PARTS),)), dma((5, len(CAND_PARTS))), dma((5, len(CAND_PARTS)))],
        **how(collective_id, 40),
        name="cand_sums",
    )(part.reshape(2, 2, 2, 2, 2, part.shape[0] // n, width))


X, Y, Z1, Z2 = 2, 4, 8, 16
PARTS = ((0, 512, (X, Y, Z1, Z2)), (512, 256, (Z1, X, Y, Z2)), (768, 512, (Y, X, Z1, Z2)), (1280, 256, (Z1, Y, X, Z2)))
GROUP = 1536


def sum_body(n, groups, srcs, note, outs, note_out, acc, got, notes, load_sem, pair_sem, half_sem, full_sem, send_sem, out_sem, note_sem):
    me = lax.axis_index("dp")
    core = lax.rem(me, 2)
    partner = me + 1 - 2 * core
    bit = {d: lax.rem(me // d, 2) for d in (X, Y, Z1, Z2)}
    across = {d: me + d * (1 - 2 * bit[d]) for d in bit}
    per_src = groups // len(srcs)
    full = got[0]
    width = acc.shape[-1]

    def area(ref, group, start, shift, size):
        high = ref.shape[0]
        if ref.shape[1] == width:
            return ref.at[pl.ds(pl.multiple_of(group * GROUP + start + shift, 8), size)]
        column = pl.multiple_of((group * (GROUP // high) + start // high) * width, width)
        return ref.at[pl.ds(pl.multiple_of(start % high + shift, 8), size), pl.ds(column, width)]

    def spot(part, level):
        start, rows, dims = part
        at, size = start // 2, rows // 2
        for d in dims[:level]:
            size //= 2
            at = at + bit[d] * size
        return at if level == 0 else pl.multiple_of(at, 8), size

    def away(part, level):
        at, size = spot(part, level)
        return pl.multiple_of(at + (1 - bit[part[2][level]]) * (size // 2), 8), size // 2

    each_other(n, me, greet)
    for g in range(groups):
        for start, rows, _ in PARTS:
            half = rows // 2
            mine = area(srcs[g // per_src], g % per_src, start, core * half, half)
            pltpu.make_async_copy(mine, acc.at[g, pl.ds(start // 2, half)], load_sem.at[g]).start()
    notes[me] = note[...]
    pl.semaphore_wait(greet(), n - 1)

    for g in range(groups):
        for start, rows, _ in PARTS:
            half = rows // 2
            other = area(srcs[g // per_src], g % per_src, start, (1 - core) * half, half)
            copy_to(other, full.at[g, pl.ds(start // 2, half)], send_sem.at[0], pair_sem.at[g], partner).start()

    each_other(n, me, lambda dev: copy_to(note, notes.at[me], note_sem.at[0], note_sem.at[1], dev).start())

    def add(dst, at, x, x_at, y, y_at, size, g):
        block = min(size, 32)

        def one(i, carry):
            k = pl.multiple_of(i * block, block)
            dst[g, pl.ds(at + k, block)] = x[g, pl.ds(x_at + k, block)] + y[g, pl.ds(y_at + k, block)]
            return carry

        lax.fori_loop(0, size // block, one, None)

    def advance(stage, g):
        if stage == 0:
            pltpu.make_async_copy(acc.at[g], acc.at[g], load_sem.at[g]).wait()
            arrived(full.at[g], pair_sem.at[g])
        for p, part in enumerate(PARTS):
            start, rows, dims = part
            if stage <= 4:
                at, size = spot(part, stage)
                in_at = start >> (stage + 1)
                if stage:
                    arrived(got[stage].at[g, pl.ds(in_at, size)], half_sem.at[stage - 1, p, g])
                if stage < 4:
                    add(acc, at, acc, at, got[stage], in_at, size, g)
                    off, half = away(part, stage)
                    copy_to(acc.at[g, pl.ds(off, half)], got[stage + 1].at[g, pl.ds(start >> (stage + 2), half)],
                            send_sem.at[stage + 1], half_sem.at[stage, p, g], across[dims[stage]]).start()
                    continue
                add(full, at, acc, at, got[stage], in_at, size, g)
            else:
                back_at, back = spot(part, 9 - stage)
                there = full.at[g, pl.ds(pl.multiple_of(back_at + (1 - 2 * bit[dims[8 - stage]]) * back, 8), back)]
                arrived(there, full_sem.at[stage - 5, p, g])
                at, size = spot(part, 8 - stage)
            if stage < 8:
                held = full.at[g, pl.ds(at, size)]
                copy_to(held, held, send_sem.at[stage + 1], full_sem.at[stage - 4, p, g], across[dims[7 - stage]]).start()
            else:
                half = rows // 2
                held = full.at[g, pl.ds(start // 2, half)]
                for i, out in enumerate(outs):
                    @pl.when(g // per_src == i)
                    def _():
                        place = area(out, lax.rem(g, per_src), start, core * half, half)
                        copy_to(held, place, send_sem.at[9], out_sem.at[0], partner).start()
                        pltpu.make_async_copy(held, place, out_sem.at[1]).start()

    def tick(k, carry):
        for stage in reversed(range(9)):
            g = k - stage
            pl.when((g >= 0) & (g < groups))(functools.partial(advance, stage, g))
        return carry

    lax.fori_loop(0, groups + 8, tick, None)

    departed(notes.at[pl.ds(0, n - 1)], note_sem.at[0])
    arrived(notes.at[pl.ds(0, n - 1)], note_sem.at[1])
    note_out[...] = jnp.sum(notes[...], axis=0)
    for i, sent in enumerate(got):
        departed(sent, send_sem.at[i])
        departed(sent, send_sem.at[9 - i])
    arrived(full, out_sem.at[0])
    pltpu.make_async_copy(full, full, out_sem.at[1]).wait()


def sum_over_devices(n, srcs, note, collective_id):
    width = min(srcs[0].shape)
    groups = len(srcs) * srcs[0].size // (GROUP * width)
    sizes = [(groups, GROUP // 2 >> i, width) for i in range(5)]

    def body(*refs):
        rest = iter(refs)
        ins, note_in = [next(rest) for _ in srcs], next(rest)
        outs, note_out = [next(rest) for _ in srcs], next(rest)
        acc, got = next(rest), [next(rest) for _ in sizes]
        sum_body(n, groups, ins, note_in, outs, note_out, acc, got, *rest)

    vmem = pl.BlockSpec(memory_space=pltpu.VMEM)
    dma = pltpu.SemaphoreType.DMA
    return pl.pallas_call(
        body,
        out_shape=tuple(jax.ShapeDtypeStruct(x.shape, jnp.float32) for x in tuple(srcs) + (note,)),
        in_specs=[ANY] * len(srcs) + [vmem],
        out_specs=(ANY,) * len(srcs) + (vmem,),
        scratch_shapes=[pltpu.VMEM(sizes[0], jnp.float32)] + [pltpu.VMEM(s, jnp.float32) for s in sizes] + [
            pltpu.VMEM((n,) + note.shape, jnp.float32),
            dma((groups,)), dma((groups,)), dma((4, len(PARTS), groups)), dma((4, len(PARTS), groups)), dma((10,)), dma((2,)), dma((2,)),
        ],
        **how(collective_id, 200),
        name="weight_sums",
    )(*srcs, note)


def comm_call(body, srcs, out_shapes, collective_id, name, sems=((), (), ())):
    return pl.pallas_call(
        body,
        out_shape=[jax.ShapeDtypeStruct(shape, srcs[0].dtype) for shape in out_shapes],
        in_specs=[ANY] * len(srcs),
        out_specs=[ANY] * len(out_shapes),
        scratch_shapes=[pltpu.SemaphoreType.DMA(shape) if shape else pltpu.SemaphoreType.DMA for shape in sems],
        **how(collective_id, 50),
        name=name,
    )(*srcs)


def solution(mesh):
    n = mesh.shape["dp"]

    def local_step(tokens, w_one, w_two, wi_one, wi_two, table_loc, cand_ids, log_q, targ_loc):
        me = lax.axis_index("dp")
        rows_loc, width = table_loc.shape
        num_tok = tokens.shape[0]
        num_cand = cand_ids.shape[0]
        cand_loc = num_cand // n
        num_req = num_tok + cand_loc
        tok_total = num_tok * n

        def swap(src, collective_id, name):
            return comm_call(functools.partial(all_to_all_body, n), [src], [src.shape], collective_id, name)[0]

        req_ids = jnp.concatenate([targ_loc, lax.dynamic_slice(cand_ids, (me * cand_loc,), (cand_loc,))])
        owner = req_ids // rows_loc
        local_id = req_ids - owner * rows_loc
        is_owner = (owner[:, None] == jnp.arange(n)[None, :]).astype(jnp.bfloat16)
        earlier = (jnp.arange(num_req)[:, None] > jnp.arange(num_req)[None, :]).astype(jnp.bfloat16)
        before = jnp.dot(earlier, is_owner, preferred_element_type=jnp.float32)
        is_owner_f = is_owner.astype(jnp.float32)
        rank = jnp.sum(before * is_owner_f, axis=1).astype(jnp.int32)
        counts = jnp.sum(is_owner_f, axis=0).astype(jnp.int32)

        depth = -(-num_req // 128) * 128
        is_rank = (rank[:, None] == jnp.arange(depth)[None, :]).astype(jnp.bfloat16)
        place = jnp.arange(num_req)
        halves = [local_id // 64, local_id % 64, place // 64, place % 64, jnp.ones_like(place)]
        picks = jnp.concatenate([is_owner * h.astype(jnp.bfloat16)[:, None] for h in halves], axis=1)
        tables = jnp.einsum("ia,ij->aj", picks, is_rank, preferred_element_type=jnp.float32).astype(jnp.int32).reshape(5, n, depth)
        want_ids = jnp.where(tables[4] > 0, tables[0] * 64 + tables[1], -1)
        places = tables[2] * 64 + tables[3]

        lines = depth // 128
        note = jnp.concatenate([
            want_ids.reshape(n, lines, 128),
            jnp.broadcast_to(jnp.pad(counts, (0, 128 - n))[None, None, :], (n, 16 - lines, 128)),
        ], axis=1)
        notes = swap(note, 0, "notes")
        ask_ids = notes[:, :lines].reshape(n, depth)
        all_counts = notes[:, lines, :n]

        most = jnp.max(all_counts)
        too_many = most > PAIR_ROWS + HOT_ROWS
        extra_rounds = jnp.where(too_many, (most + PAIR_ROWS - 1) // PAIR_ROWS - 1, 0)
        hot_chip = jnp.max(all_counts.reshape(n, n // 2, 2), axis=(0, 2)) > PAIR_ROWS
        num_hot = jnp.sum(hot_chip.astype(jnp.int32))
        hot_rank = jnp.sum((jnp.arange(n // 2)[None, :] < jnp.arange(n // 2)[:, None]) & hot_chip[None, :], axis=1)

        def hot_at(i):
            return jnp.sum(jnp.where(hot_chip & (hot_rank == i), jnp.arange(n // 2), 0))

        ask_pad = jnp.pad(ask_ids, ((0, 0), (0, HOT_ROWS)), constant_values=-1)
        place_pad = jnp.pad(places, ((0, 0), (0, HOT_ROWS)))

        def window(table, at, size):
            return lax.dynamic_slice(table, (0, at), (table.shape[0], size))

        def fetch(ids):
            picked = jnp.take(table_loc, ids.reshape(-1), axis=0, mode="clip")
            return picked.reshape(ids.shape + (width,))

        rows_out_src = fetch(ask_ids[:, :PAIR_ROWS])
        none = n // 2

        slot = 2 * rows_loc + owner * PAIR_ROWS + rank

        def come_in(i, rows):
            chip = jnp.where(i < num_hot, hot_at(i), none)

            def from_root(root):
                sems = ((), (), (), (3, 4), (3, -(-CHUNKS // 3)), (), (), (), ())
                return lambda src, table: comm_call(functools.partial(rows_in_body, n, root), [src, table], [(2 * rows_loc + n * PAIR_ROWS, width)], 4 + root, f"rows_in_{root}", sems)[0]

            got = lax.switch(chip, [from_root(k) for k in range(none + 1)], rows_out_src, table_loc)
            here = owner // 2 == chip
            at = jnp.where(here, lax.rem(owner, 2) * rows_loc + local_id, slot)
            return jnp.where((here | (i == 0))[:, None], jnp.take(got, at, axis=0, mode="clip"), rows)

        raw = lax.fori_loop(0, jnp.maximum(num_hot, 1), come_in, jnp.zeros((num_req, width), jnp.bfloat16))

        cand_vec = lax.all_gather(tower_fwd(raw[num_tok:], wi_one, wi_two)[2], "dp", axis=0, tiled=True)
        i_pre, i_hidden, i_vec = tower_fwd(raw, wi_one, wi_two)
        targ_vec = i_vec[:num_tok]
        q_pre, q_hidden, query = tower_fwd(tokens, w_one, w_two)
        loss_sum, d_query, d_targ_vec, dz_cand, logit_scale = loss_grads(query, targ_vec, cand_vec, log_q, targ_loc, cand_ids, tok_total)
        d_cand_part = jnp.einsum("ts,td->sd", dz_cand, query, preferred_element_type=jnp.float32)
        dw_one, dw_two = tower_back(tokens, w_two, q_pre, q_hidden, d_query)[1:]
        d_cand_part, dw_one, dw_two = lax.optimization_barrier((d_cand_part, dw_one, dw_two))
        query_sums = lax.psum((dw_one, dw_two), "dp")
        d_cand_vec = (cand_sum(n, d_cand_part, 3) * logit_scale).astype(jnp.bfloat16)
        d_vec = jnp.concatenate([d_targ_vec, d_cand_vec])
        i_grad_pre, dwi_one, dwi_two = tower_back(raw, wi_two, i_pre, i_hidden, d_vec)
        d_raw = jnp.einsum("nf,df->nd", i_grad_pre, wi_one, preferred_element_type=jnp.float32).astype(jnp.bfloat16)
        def spread(ids):
            return jnp.take(d_raw, ids.reshape(-1), axis=0, mode="clip").reshape(ids.shape + (width,))

        def add_rows(acc, ids, rows):
            ids = ids.reshape(-1)
            ids = jnp.where(ids >= 0, ids, rows_loc)
            return acc.at[ids].add(rows.reshape(-1, width).astype(jnp.float32), mode="drop")

        cold_src = spread(places[:, :PAIR_ROWS])
        out_ids = ask_ids[:, :PAIR_ROWS + HOT_ROWS].reshape(n, SLICES + 1, PAIR_ROWS)
        out_ids = out_ids.transpose(1, 0, 2).reshape(SLICES + 1, 1, n * PAIR_ROWS)
        first = jnp.arange(SLICES + 1)[:, None, None] == 0
        hot_back = jnp.where(too_many, 0, num_hot)

        def go_out(i, acc):
            chip = jnp.where(i < hot_back, hot_at(i), none)
            hot_places = lax.dynamic_slice(places, (2 * jnp.minimum(chip, none - 1), PAIR_ROWS), (2, HOT_ROWS))
            hot_places = hot_places.reshape(2, SLICES, PAIR_ROWS).transpose(1, 0, 2)

            def to_root(root):
                return lambda *args: rows_out(n, root, *args, 4 + n + root)

            return lax.switch(chip, [to_root(k) for k in range(none + 1)], cold_src, spread(hot_places), jnp.where(first & (i > 0), -1, out_ids), acc)

        d_table = lax.fori_loop(0, jnp.maximum(hot_back, 1), go_out, jnp.zeros((rows_loc, width), jnp.float32))

        def extra_out(r, acc):
            back = swap(spread(window(place_pad, r * PAIR_ROWS, PAIR_ROWS)), 1, "rows_more")
            return add_rows(acc, window(ask_pad, r * PAIR_ROWS, PAIR_ROWS), back)

        d_table = lax.fori_loop(1, 1 + extra_rounds, extra_out, d_table)
        loss_note, d_table = lax.optimization_barrier((jnp.full((8, 128), loss_sum, jnp.float32), d_table))
        dwi_one, dwi_two, loss_note = sum_over_devices(n, (dwi_one, dwi_two), loss_note, 2)
        loss = loss_note[0, 0] / tok_total
        return loss, d_table, query_sums[0], query_sums[1], dwi_one, dwi_two

    return jax.shard_map(local_step, mesh=mesh, in_specs=(P("dp", None), P(), P(), P(), P(), P("dp", None), P(), P(), P("dp")), out_specs=(P(), P("dp", None), P(), P(), P(), P()), check_vma=False)
```

```python
import functools
import math
import jax
import jax.numpy as jnp
from jax import lax
from jax.experimental import pallas as pl
from jax.experimental.pallas import tpu as pltpu
from jax.sharding import PartitionSpec as P

SCORE_GAIN = 3.0
HIT_VALUE = -1e9
PAIR_ROWS = 48
SLICES = 5
HOT_ROWS = SLICES * PAIR_ROWS
CHUNKS = 128
LAG = 3
MESH = pl.DeviceIdType.MESH
ANY = pl.BlockSpec(memory_space=pl.ANY)


def tower_fwd(row_block, w_in, w_out):
    pre_act = jnp.dot(row_block, w_in, preferred_element_type=jnp.float32)
    hidden = jax.nn.gelu(pre_act).astype(jnp.bfloat16)
    tower_out = jnp.dot(hidden, w_out, preferred_element_type=jnp.float32).astype(jnp.bfloat16)
    return pre_act, hidden, tower_out


def tower_back(row_block, w_out, pre_act, hidden, grad_out):
    dw_out = jnp.einsum("nf,nd->fd", hidden, grad_out, preferred_element_type=jnp.float32)
    grad_hidden = jnp.einsum("nd,fd->nf", grad_out, w_out, preferred_element_type=jnp.float32)
    gelu_back = jax.vjp(jax.nn.gelu, pre_act)[1]
    grad_pre = gelu_back(grad_hidden)[0].astype(jnp.bfloat16)
    dw_in = jnp.einsum("ne,nf->ef", row_block, grad_pre, preferred_element_type=jnp.float32)
    return grad_pre, dw_in, dw_out


def loss_grads(query, targ_vec, cand_vec, log_q, targ_ids, cand_ids, tok_total):
    logit_scale = SCORE_GAIN / math.sqrt(query.shape[1])
    z_targ = jnp.einsum("td,td->t", query, targ_vec, preferred_element_type=jnp.float32) * logit_scale
    z_cand = jnp.einsum("td,sd->ts", query, cand_vec, preferred_element_type=jnp.float32) * logit_scale - log_q[None, :]
    z_cand = jnp.where(targ_ids[:, None] == cand_ids[None, :], HIT_VALUE, z_cand)
    row_max = jnp.maximum(z_targ, jnp.max(z_cand, axis=1))
    e_targ = jnp.exp(z_targ - row_max)
    e_cand = jnp.exp(z_cand - row_max[:, None])
    denom_sum = e_targ + jnp.sum(e_cand, axis=1)
    loss_sum = jnp.sum(jnp.log(denom_sum) + row_max - z_targ)
    dz_targ = ((e_targ / denom_sum - 1.0) / tok_total).astype(jnp.bfloat16).astype(jnp.float32)
    dz_cand = (e_cand / denom_sum[:, None] / tok_total).astype(jnp.bfloat16)
    d_query = ((dz_targ[:, None] * targ_vec.astype(jnp.float32) + jnp.einsum("ts,sd->td", dz_cand, cand_vec, preferred_element_type=jnp.float32)) * logit_scale).astype(jnp.bfloat16)
    d_targ_vec = (logit_scale * dz_targ[:, None] * query.astype(jnp.float32)).astype(jnp.bfloat16)
    return loss_sum, d_query, d_targ_vec, dz_cand, logit_scale


def how(collective_id, us, mib=34):
    return dict(
        compiler_params=pltpu.CompilerParams(collective_id=collective_id, has_side_effects=True, vmem_limit_bytes=mib << 20),
        cost_estimate=pl.CostEstimate(flops=us * 30_000_000, bytes_accessed=0, transcendentals=0),
    )


def copy_to(src, dst, send_sem, recv_sem, dev):
    return pltpu.make_async_remote_copy(src, dst, send_sem, recv_sem, device_id=(dev,), device_id_type=MESH)


def greet(*devs):
    barrier = pltpu.get_barrier_semaphore()
    for dev in devs:
        pl.semaphore_signal(barrier, device_id=(dev,), device_id_type=MESH)
    return barrier


def each_other(n, me, act):
    def one(i, carry):
        act(lax.rem(me + i, n))
        return carry

    lax.fori_loop(1, n, one, None)


def arrived(ref, sem):
    copy_to(ref, ref, sem, sem, lax.axis_index("dp")).wait_recv()


def departed(ref, sem):
    copy_to(ref, ref, sem, sem, lax.axis_index("dp")).wait_send()


def swap_start(n, me, src, place, send_sem, recv_sem, own_sem):
    pltpu.make_async_copy(src.at[me], place(me), own_sem).start()
    each_other(n, me, lambda dev: copy_to(src.at[dev], place(me), send_sem, recv_sem, dev).start())


def swap_end(n, me, src, send_sem, recv_sem, own_sem):
    pltpu.make_async_copy(src.at[me], src.at[me], own_sem).wait()
    departed(src.at[pl.ds(0, n - 1)], send_sem)
    arrived(src.at[pl.ds(0, n - 1)], recv_sem)


def all_to_all_body(n, src, dst, *sems):
    me = lax.axis_index("dp")
    each_other(n, me, greet)
    pl.semaphore_wait(greet(), n - 1)
    swap_start(n, me, src, lambda s: dst.at[s], *sems)
    swap_end(n, me, src, *sems)


TREES = (
    ((4368, 13104, 273, 224), (17476, 52425, 1092, 0), (43689, 2, 2730, 0)),
    ((4353, 13059, 284, 528), (17476, 52380, 1088, 64), (43674, 32, 2720, 160)),
)


def tree_depths(masks, start, chips):
    depth = {start: 0}
    while len(depth) < chips:
        for c, at in tuple(depth.items()):
            for d, to in enumerate((c ^ 1, c ^ 2, c + 4, c - 4)):
                if masks[d] >> c & 1:
                    depth[to] = at + 1
    return depth


def rows_in_body(n, root, src, table, dst, send_sem, recv_sem, own_sem, *sems):
    me = lax.axis_index("dp")
    high, size = table.shape[0], src.shape[1]
    each_other(n, me, greet)
    pl.semaphore_wait(greet(), n - 1)
    swap_start(n, me, src, lambda s: dst.at[pl.ds(pl.multiple_of(2 * high + s * size, 16), size)], send_sem, recv_sem, own_sem)
    if root < n // 2:
        broadcast(n, root, table, lambda core: dst.at[pl.ds(pl.multiple_of(core * high, high), high)], *sems)
    swap_end(n, me, src, send_sem, recv_sem, own_sem)


def broadcast(n, root, src, dst, send_sem, recv_sem, pair_send, pair_recv, echo_send, echo_recv):
    me = lax.axis_index("dp")
    core = lax.rem(me, 2)
    chip = me // 2
    at_x, at_y, at_z = lax.rem(chip, 2), lax.rem(chip // 2, 2), chip // 4
    root_z = root // 4
    up = 1 if root_z < 2 else -1
    rel_z = at_z if root_z < 2 else 3 - at_z
    rel = (rel_z * 2 + lax.rem(at_y + root // 2, 2)) * 2 + lax.rem(at_x + root, 2)
    is_root = chip == root
    trees = TREES[min(root_z, 3 - root_z)]
    to = (me + 2 - 4 * at_x, me + 4 - 8 * at_y, me + 8 * up, me - 8 * up)
    partner = me + 1 - 2 * core

    def passes(mask):
        hit = rel < 0
        for c in range(n // 2):
            if mask >> c & 1:
                hit = hit | (rel == c)
        return hit

    moves = [[(d, passes(trees[t][d])) for d in range(4) if trees[t][d]] for t in range(3)]
    depths = [tree_depths(trees[t], 4 * min(root_z, 3 - root_z), n // 2) for t in range(3)]
    behind = [LAG * sum((rel == c).astype(jnp.int32) * depths[t][c] for c in range(n // 2)) for t in range(3)]

    rows = src.shape[0] // CHUNKS
    steps = -(-CHUNKS // 3)

    def step(held, j, t):
        piece = pl.ds((3 * j + t) * rows, rows)
        for d, on in moves[t]:
            @pl.when(on)
            def _():
                copy_to(held.at[piece], dst(core).at[piece], send_sem.at[t, d], recv_sem.at[t, j], to[d]).start()

    @pl.when(is_root)
    def _():
        copy_to(src, dst(core), pair_send, pair_recv, partner).start()

        def go(j, carry):
            for t in range(3):
                pl.when(3 * j + t < CHUNKS)(functools.partial(step, src, j, t))
            return carry

        lax.fori_loop(0, steps, go, None)
        arrived(dst(1 - core), pair_recv)
        copy_to(dst(1 - core), dst(1 - core), echo_send, echo_recv, partner).start()
        copy_to(dst(core), dst(core), echo_send, echo_recv, partner).wait()

    @pl.when(jnp.logical_not(is_root))
    def _():
        held = dst(core)

        def relay(t, j):
            piece = pl.ds((3 * j + t) * rows, rows)
            arrived(held.at[piece], recv_sem.at[t, j])
            step(held, j, t)
            copy_to(held.at[piece], dst(core).at[piece], pair_send, pair_recv, partner).start()

        def go(i, carry):
            for t in range(3):
                j = i - behind[t]
                pl.when((j >= 0) & (3 * j + t < CHUNKS))(functools.partial(relay, t, j))
            return carry

        far = max(max(d.values()) for d in depths)
        lax.fori_loop(LAG, steps + LAG * far, go, None)
        arrived(held, pair_recv)

    departed(src, pair_send)
    for t in range(3):
        part = pl.ds(0, len(range(t, CHUNKS, 3)) * rows)
        for d, on in moves[t]:
            @pl.when(on)
            def _():
                departed(src.at[part], send_sem.at[t, d])


def rows_out_body(n, root, src, hot_src, ids, table, table_out, rows, relay, acc, pick, send_sem, recv_sem, own_sem, relay_sem, load_sem):
    me = lax.axis_index("dp")
    core, chip = lax.rem(me, 2), me // 2
    is_root = chip == root
    slices, _, size, width = hot_src.shape
    block, depth = pick.shape
    wide = 256
    blocks = acc.shape[0] // block
    others = pl.ds(0, (n - 1) * size)

    def place(s):
        return pl.ds(pl.multiple_of(s * size, size), size)

    def take(k):
        arrived(rows.at[k, others], recv_sem.at[k])
        pltpu.make_async_copy(src.at[me], rows.at[k, place(me)], own_sem.at[k]).wait()

        def add(i, carry):
            start = pl.multiple_of(lax.rem(i, blocks) * block, block)
            deep = pl.ds(pl.multiple_of(i // blocks * depth, depth), depth)
            row = lax.broadcasted_iota(jnp.int32, (block, depth), 0) + start
            pick[...] = (row == ids[k, :, deep]).astype(jnp.float32).astype(jnp.bfloat16)

            def columns(w, carry):
                part = pl.ds(pl.multiple_of(w * wide, wide), wide)
                acc[pl.ds(start, block), part] += jnp.dot(pick[...], rows[k, deep, part], preferred_element_type=jnp.float32)
                return carry

            return lax.fori_loop(0, width // wide, columns, carry)

        lax.fori_loop(0, blocks * (n * size // depth), add, None)

    each_other(n, me, greet)
    load = pltpu.make_async_copy(table, acc, load_sem)
    load.start()
    pl.semaphore_wait(greet(), n - 1)
    if root < n // 2:
        off_x, off_y = lax.rem(chip + root, 2), lax.rem(chip // 2 + root // 2, 2)
        aside = me + 4 - 8 * lax.rem(chip // 2, 2)
        on_turn = (off_x == 1) & (lax.rem(me // 8, 2) == 1)
        goes_aside, relays = on_turn & (off_y == 1), on_turn & (off_y == 0)

        @pl.when(is_root)
        def _():
            for k in range(slices):
                copy_to(hot_src.at[k, 1 - core], rows.at[k + 1, place(me)], send_sem.at[1], recv_sem.at[k + 1], me + 1 - 2 * core).start()
                pltpu.make_async_copy(hot_src.at[k, core], rows.at[k + 1, place(me)], own_sem.at[k + 1]).start()

        @pl.when(goes_aside)
        def _():
            for k in range(slices):
                copy_to(hot_src.at[k], relay.at[k], send_sem.at[1], relay_sem.at[k], aside).start()

        @pl.when(jnp.logical_not(is_root | goes_aside))
        def _():
            for k in range(slices):
                for to in range(2):
                    copy_to(hot_src.at[k, to], rows.at[k + 1, place(me)], send_sem.at[1], recv_sem.at[k + 1], 2 * root + to).start()

    pltpu.make_async_copy(src.at[me], rows.at[0, place(me)], own_sem.at[0]).start()
    each_other(n, me, lambda dev: copy_to(src.at[dev], rows.at[0, place(me)], send_sem.at[0], recv_sem.at[0], dev).start())
    if root < n // 2:
        @pl.when(relays)
        def _():
            for k in range(slices):
                arrived(relay.at[k], relay_sem.at[k])
                for to in range(2):
                    copy_to(relay.at[k, to], rows.at[k + 1, place(aside)], send_sem.at[2], recv_sem.at[k + 1], 2 * root + to).start()

    load.wait()

    def take_if_mine(k, carry):
        k = lax.rem(k, slices + 1)
        pl.when((k == 0) | is_root)(functools.partial(take, k))
        return carry

    lax.fori_loop(1 if root < n // 2 else slices + 1, slices + 2, take_if_mine, None)
    store = pltpu.make_async_copy(acc, table_out, load_sem)
    store.start()
    departed(rows.at[0, others], send_sem.at[0])
    if root < n // 2:
        @pl.when(is_root)
        def _():
            departed(hot_src.at[:, 0], send_sem.at[1])

        @pl.when(jnp.logical_not(is_root))
        def _():
            departed(hot_src, send_sem.at[1])

        @pl.when(relays)
        def _():
            departed(relay, send_sem.at[2])

    store.wait()


def rows_out(n, root, src, hot_src, ids, table, collective_id):
    slices, _, size, width = hot_src.shape
    dma = pltpu.SemaphoreType.DMA
    shapes = ((slices + 1, n * size, width), hot_src.shape, table.shape, (1024, 512))
    return pl.pallas_call(
        functools.partial(rows_out_body, n, root),
        out_shape=jax.ShapeDtypeStruct(table.shape, table.dtype),
        in_specs=[ANY, ANY, pl.BlockSpec(memory_space=pltpu.VMEM), ANY],
        out_specs=ANY,
        input_output_aliases={3: 0},
        scratch_shapes=[pltpu.VMEM(shape, table.dtype if shape == table.shape else src.dtype) for shape in shapes]
        + [dma((3,)), dma((slices + 1,)), dma((slices + 1,)), dma((slices,)), dma],
        **how(collective_id, 150),
        name=f"rows_out_{root}",
    )(src, hot_src, ids, table)


CAND_PARTS = ((0, 24, (3, 2, 1, 0)), (24, 24, (2, 3, 1, 0)), (48, 8, (1, 3, 2, 0)), (56, 8, (1, 2, 3, 0)))


def cand_sum_body(n, src, out, *refs):
    num = len(CAND_PARTS)
    acc, refs = refs[:num], refs[num:]
    got, (load_sem, recv_sem, send_sem) = [refs[i * num:(i + 1) * num] for i in range(5)], refs[5 * num:]
    me = lax.axis_index("dp")
    core = lax.rem(me, 2)
    bit = [lax.rem(me // d, 2) for d in (16, 8, 4, 2)]
    across = [me + d * (1 - 2 * b) for d, b in zip((16, 8, 4, 2), bit)]
    partner = me + 1 - 2 * core
    every = slice(None)

    pl.semaphore_wait(greet(partner, *across), 5)

    for p, (at, rows, _) in enumerate(CAND_PARTS):
        w = pl.ds(at, rows)
        copy_to(src.at[:, :, :, :, 1 - core, w], got[0][p], send_sem.at[0, p], recv_sem.at[0, p], partner).start()
        pltpu.make_async_copy(src.at[:, :, :, :, core, w], acc[p], load_sem.at[p]).start()

    def add(p, level, fixed):
        held = CAND_PARTS[p][2][:level]
        free = [a for a in range(4) if fixed[a] is every]
        for k in range(2 ** len(free)):
            index = list(fixed)
            for j, a in enumerate(free):
                index[a] = k >> j & 1
            there = tuple(index[a] for a in range(4) if a not in held)
            acc[p][tuple(index)] += got[level][p][there]

    for level in range(5):
        for p, (at, rows, dims) in enumerate(CAND_PARTS):
            if level == 0:
                pltpu.make_async_copy(acc[p], acc[p], load_sem.at[p]).wait()
            arrived(got[level][p], recv_sem.at[level, p])
            fixed = [bit[a] if a in dims[:level] else every for a in range(4)]
            if level == 4:
                out[pl.ds(at, rows)] = acc[p][tuple(fixed)] + got[4][p][...]
                continue
            axis = dims[level]
            away, kept = list(fixed), list(fixed)
            away[axis], kept[axis] = 1 - bit[axis], bit[axis]
            add(p, level, away)
            copy_to(acc[p].at[tuple(away)], got[level + 1][p], send_sem.at[level + 1, p], recv_sem.at[level + 1, p], across[axis]).start()
            add(p, level, kept)
    for level in range(5):
        for p in range(num):
            departed(got[level][p], send_sem.at[level, p])


def cand_sum(n, part, collective_id):
    width = part.shape[1]
    dma = pltpu.SemaphoreType.DMA
    sizes = [[(2,) * (4 - level) + (rows, width) for _, rows, _ in CAND_PARTS] for level in range(5)]
    return pl.pallas_call(
        functools.partial(cand_sum_body, n),
        out_shape=jax.ShapeDtypeStruct((part.shape[0] // n, width), part.dtype),
        in_specs=[ANY],
        out_specs=pl.BlockSpec(memory_space=pltpu.VMEM),
        scratch_shapes=[pltpu.VMEM(s, part.dtype) for level in [0] + list(range(5)) for s in sizes[level]] + [dma((len(CAND_PARTS),)), dma((5, len(CAND_PARTS))), dma((5, len(CAND_PARTS)))],
        **how(collective_id, 40),
        name="cand_sums",
    )(part.reshape(2, 2, 2, 2, 2, part.shape[0] // n, width))


X, Y, Z1, Z2 = 2, 4, 8, 16
PARTS = ((0, 512, (X, Y, Z1, Z2)), (512, 256, (Z1, X, Y, Z2)), (768, 512, (Y, X, Z1, Z2)), (1280, 256, (Z1, Y, X, Z2)))
GROUP = 1536


def sum_body(n, groups, srcs, note, outs, note_out, acc, got, notes, load_sem, pair_sem, half_sem, full_sem, send_sem, out_sem, note_sem):
    me = lax.axis_index("dp")
    core = lax.rem(me, 2)
    partner = me + 1 - 2 * core
    bit = {d: lax.rem(me // d, 2) for d in (X, Y, Z1, Z2)}
    across = {d: me + d * (1 - 2 * bit[d]) for d in bit}
    per_src = groups // len(srcs)
    full = got[0]
    width = acc.shape[-1]

    def area(ref, group, start, shift, size):
        high = ref.shape[0]
        if ref.shape[1] == width:
            return ref.at[pl.ds(pl.multiple_of(group * GROUP + start + shift, 8), size)]
        column = pl.multiple_of((group * (GROUP // high) + start // high) * width, width)
        return ref.at[pl.ds(pl.multiple_of(start % high + shift, 8), size), pl.ds(column, width)]

    def spot(part, level):
        start, rows, dims = part
        at, size = start // 2, rows // 2
        for d in dims[:level]:
            size //= 2
            at = at + bit[d] * size
        return at if level == 0 else pl.multiple_of(at, 8), size

    def away(part, level):
        at, size = spot(part, level)
        return pl.multiple_of(at + (1 - bit[part[2][level]]) * (size // 2), 8), size // 2

    each_other(n, me, greet)
    for g in range(groups):
        for start, rows, _ in PARTS:
            half = rows // 2
            mine = area(srcs[g // per_src], g % per_src, start, core * half, half)
            pltpu.make_async_copy(mine, acc.at[g, pl.ds(start // 2, half)], load_sem.at[g]).start()
    notes[me] = note[...]
    pl.semaphore_wait(greet(), n - 1)

    for g in range(groups):
        for start, rows, _ in PARTS:
            half = rows // 2
            other = area(srcs[g // per_src], g % per_src, start, (1 - core) * half, half)
            copy_to(other, full.at[g, pl.ds(start // 2, half)], send_sem.at[0], pair_sem.at[g], partner).start()

    each_other(n, me, lambda dev: copy_to(note, notes.at[me], note_sem.at[0], note_sem.at[1], dev).start())

    def add(dst, at, x, x_at, y, y_at, size, g):
        block = min(size, 32)

        def one(i, carry):
            k = pl.multiple_of(i * block, block)
            dst[g, pl.ds(at + k, block)] = x[g, pl.ds(x_at + k, block)] + y[g, pl.ds(y_at + k, block)]
            return carry

        lax.fori_loop(0, size // block, one, None)

    def advance(stage, g):
        if stage == 0:
            pltpu.make_async_copy(acc.at[g], acc.at[g], load_sem.at[g]).wait()
            arrived(full.at[g], pair_sem.at[g])
        for p, part in enumerate(PARTS):
            start, rows, dims = part
            if stage <= 4:
                at, size = spot(part, stage)
                in_at = start >> (stage + 1)
                if stage:
                    arrived(got[stage].at[g, pl.ds(in_at, size)], half_sem.at[stage - 1, p, g])
                if stage < 4:
                    add(acc, at, acc, at, got[stage], in_at, size, g)
                    off, half = away(part, stage)
                    copy_to(acc.at[g, pl.ds(off, half)], got[stage + 1].at[g, pl.ds(start >> (stage + 2), half)],
                            send_sem.at[stage + 1], half_sem.at[stage, p, g], across[dims[stage]]).start()
                    continue
                add(full, at, acc, at, got[stage], in_at, size, g)
            else:
                back_at, back = spot(part, 9 - stage)
                there = full.at[g, pl.ds(pl.multiple_of(back_at + (1 - 2 * bit[dims[8 - stage]]) * back, 8), back)]
                arrived(there, full_sem.at[stage - 5, p, g])
                at, size = spot(part, 8 - stage)
            if stage < 8:
                held = full.at[g, pl.ds(at, size)]
                copy_to(held, held, send_sem.at[stage + 1], full_sem.at[stage - 4, p, g], across[dims[7 - stage]]).start()
            else:
                half = rows // 2
                held = full.at[g, pl.ds(start // 2, half)]
                for i, out in enumerate(outs):
                    @pl.when(g // per_src == i)
                    def _():
                        place = area(out, lax.rem(g, per_src), start, core * half, half)
                        copy_to(held, place, send_sem.at[9], out_sem.at[0], partner).start()
                        pltpu.make_async_copy(held, place, out_sem.at[1]).start()

    def tick(k, carry):
        for stage in reversed(range(9)):
            g = k - stage
            pl.when((g >= 0) & (g < groups))(functools.partial(advance, stage, g))
        return carry

    lax.fori_loop(0, groups + 8, tick, None)

    departed(notes.at[pl.ds(0, n - 1)], note_sem.at[0])
    arrived(notes.at[pl.ds(0, n - 1)], note_sem.at[1])
    note_out[...] = jnp.sum(notes[...], axis=0)
    for i, sent in enumerate(got):
        departed(sent, send_sem.at[i])
        departed(sent, send_sem.at[9 - i])
    arrived(full, out_sem.at[0])
    pltpu.make_async_copy(full, full, out_sem.at[1]).wait()


def sum_over_devices(n, srcs, note, collective_id):
    width = min(srcs[0].shape)
    groups = len(srcs) * srcs[0].size // (GROUP * width)
    sizes = [(groups, GROUP // 2 >> i, width) for i in range(5)]

    def body(*refs):
        rest = iter(refs)
        ins, note_in = [next(rest) for _ in srcs], next(rest)
        outs, note_out = [next(rest) for _ in srcs], next(rest)
        acc, got = next(rest), [next(rest) for _ in sizes]
        sum_body(n, groups, ins, note_in, outs, note_out, acc, got, *rest)

    vmem = pl.BlockSpec(memory_space=pltpu.VMEM)
    dma = pltpu.SemaphoreType.DMA
    return pl.pallas_call(
        body,
        out_shape=tuple(jax.ShapeDtypeStruct(x.shape, jnp.float32) for x in tuple(srcs) + (note,)),
        in_specs=[ANY] * len(srcs) + [vmem],
        out_specs=(ANY,) * len(srcs) + (vmem,),
        scratch_shapes=[pltpu.VMEM(sizes[0], jnp.float32)] + [pltpu.VMEM(s, jnp.float32) for s in sizes] + [
            pltpu.VMEM((n,) + note.shape, jnp.float32),
            dma((groups,)), dma((groups,)), dma((4, len(PARTS), groups)), dma((4, len(PARTS), groups)), dma((10,)), dma((2,)), dma((2,)),
        ],
        **how(collective_id, 200, 48),
        name="weight_sums",
    )(*srcs, note)


def comm_call(body, srcs, out_shapes, collective_id, name, sems=((), (), ())):
    return pl.pallas_call(
        body,
        out_shape=[jax.ShapeDtypeStruct(shape, srcs[0].dtype) for shape in out_shapes],
        in_specs=[ANY] * len(srcs),
        out_specs=[ANY] * len(out_shapes),
        scratch_shapes=[pltpu.SemaphoreType.DMA(shape) if shape else pltpu.SemaphoreType.DMA for shape in sems],
        **how(collective_id, 50),
        name=name,
    )(*srcs)


def solution(mesh):
    n = mesh.shape["dp"]

    def local_step(tokens, w_one, w_two, wi_one, wi_two, table_loc, cand_ids, log_q, targ_loc):
        me = lax.axis_index("dp")
        rows_loc, width = table_loc.shape
        num_tok = tokens.shape[0]
        num_cand = cand_ids.shape[0]
        cand_loc = num_cand // n
        num_req = num_tok + cand_loc
        tok_total = num_tok * n

        def swap(src, collective_id, name):
            return comm_call(functools.partial(all_to_all_body, n), [src], [src.shape], collective_id, name)[0]

        req_ids = jnp.concatenate([targ_loc, lax.dynamic_slice(cand_ids, (me * cand_loc,), (cand_loc,))])
        owner = req_ids // rows_loc
        local_id = req_ids - owner * rows_loc
        is_owner = (owner[:, None] == jnp.arange(n)[None, :]).astype(jnp.bfloat16)
        earlier = (jnp.arange(num_req)[:, None] > jnp.arange(num_req)[None, :]).astype(jnp.bfloat16)
        before = jnp.dot(earlier, is_owner, preferred_element_type=jnp.float32)
        is_owner_f = is_owner.astype(jnp.float32)
        rank = jnp.sum(before * is_owner_f, axis=1).astype(jnp.int32)
        counts = jnp.sum(is_owner_f, axis=0).astype(jnp.int32)

        depth = -(-num_req // 128) * 128
        is_rank = (rank[:, None] == jnp.arange(depth)[None, :]).astype(jnp.bfloat16)
        place = jnp.arange(num_req)
        halves = [local_id // 64, local_id % 64, place // 64, place % 64, jnp.ones_like(place)]
        picks = jnp.concatenate([is_owner * h.astype(jnp.bfloat16)[:, None] for h in halves], axis=1)
        tables = jnp.einsum("ia,ij->aj", picks, is_rank, preferred_element_type=jnp.float32).astype(jnp.int32).reshape(5, n, depth)
        want_ids = jnp.where(tables[4] > 0, tables[0] * 64 + tables[1], -1)
        places = tables[2] * 64 + tables[3]

        lines = depth // 128
        note = jnp.concatenate([
            want_ids.reshape(n, lines, 128),
            jnp.broadcast_to(jnp.pad(counts, (0, 128 - n))[None, None, :], (n, 16 - lines, 128)),
        ], axis=1)
        notes = swap(note, 0, "notes")
        ask_ids = notes[:, :lines].reshape(n, depth)
        all_counts = notes[:, lines, :n]

        most = jnp.max(all_counts)
        too_many = most > PAIR_ROWS + HOT_ROWS
        extra_rounds = jnp.where(too_many, (most + PAIR_ROWS - 1) // PAIR_ROWS - 1, 0)
        hot_chip = jnp.max(all_counts.reshape(n, n // 2, 2), axis=(0, 2)) > PAIR_ROWS
        num_hot = jnp.sum(hot_chip.astype(jnp.int32))
        hot_rank = jnp.sum((jnp.arange(n // 2)[None, :] < jnp.arange(n // 2)[:, None]) & hot_chip[None, :], axis=1)

        def hot_at(i):
            return jnp.sum(jnp.where(hot_chip & (hot_rank == i), jnp.arange(n // 2), 0))

        ask_pad = jnp.pad(ask_ids, ((0, 0), (0, HOT_ROWS)), constant_values=-1)
        place_pad = jnp.pad(places, ((0, 0), (0, HOT_ROWS)))

        def window(table, at, size):
            return lax.dynamic_slice(table, (0, at), (table.shape[0], size))

        def fetch(ids):
            picked = jnp.take(table_loc, ids.reshape(-1), axis=0, mode="clip")
            return picked.reshape(ids.shape + (width,))

        rows_out_src = fetch(ask_ids[:, :PAIR_ROWS])
        none = n // 2

        slot = 2 * rows_loc + owner * PAIR_ROWS + rank

        def come_in(i, rows):
            chip = jnp.where(i < num_hot, hot_at(i), none)

            def from_root(root):
                sems = ((), (), (), (3, 4), (3, -(-CHUNKS // 3)), (), (), (), ())
                return lambda src, table: comm_call(functools.partial(rows_in_body, n, root), [src, table], [(2 * rows_loc + n * PAIR_ROWS, width)], 4 + root, f"rows_in_{root}", sems)[0]

            got = lax.switch(chip, [from_root(k) for k in range(none + 1)], rows_out_src, table_loc)
            here = owner // 2 == chip
            at = jnp.where(here, lax.rem(owner, 2) * rows_loc + local_id, slot)
            return jnp.where((here | (i == 0))[:, None], jnp.take(got, at, axis=0, mode="clip"), rows)

        raw = lax.fori_loop(0, jnp.maximum(num_hot, 1), come_in, jnp.zeros((num_req, width), jnp.bfloat16))

        cand_vec = lax.all_gather(tower_fwd(raw[num_tok:], wi_one, wi_two)[2], "dp", axis=0, tiled=True)
        i_pre, i_hidden, i_vec = tower_fwd(raw, wi_one, wi_two)
        targ_vec = i_vec[:num_tok]
        q_pre, q_hidden, query = tower_fwd(tokens, w_one, w_two)
        loss_sum, d_query, d_targ_vec, dz_cand, logit_scale = loss_grads(query, targ_vec, cand_vec, log_q, targ_loc, cand_ids, tok_total)
        d_cand_part = jnp.einsum("ts,td->sd", dz_cand, query, preferred_element_type=jnp.float32)
        dw_one, dw_two = tower_back(tokens, w_two, q_pre, q_hidden, d_query)[1:]
        d_cand_part, dw_two = lax.optimization_barrier((d_cand_part, dw_two))
        dw_two = lax.psum(dw_two, "dp")
        d_cand_vec = (cand_sum(n, d_cand_part, 3) * logit_scale).astype(jnp.bfloat16)
        d_vec = jnp.concatenate([d_targ_vec, d_cand_vec])
        i_grad_pre, dwi_one, dwi_two = tower_back(raw, wi_two, i_pre, i_hidden, d_vec)
        d_raw = jnp.einsum("nf,df->nd", i_grad_pre, wi_one, preferred_element_type=jnp.float32).astype(jnp.bfloat16)
        def spread(ids):
            return jnp.take(d_raw, ids.reshape(-1), axis=0, mode="clip").reshape(ids.shape + (width,))

        def add_rows(acc, ids, rows):
            ids = ids.reshape(-1)
            ids = jnp.where(ids >= 0, ids, rows_loc)
            return acc.at[ids].add(rows.reshape(-1, width).astype(jnp.float32), mode="drop")

        cold_src = spread(places[:, :PAIR_ROWS])
        out_ids = ask_ids[:, :PAIR_ROWS + HOT_ROWS].reshape(n, SLICES + 1, PAIR_ROWS)
        out_ids = out_ids.transpose(1, 0, 2).reshape(SLICES + 1, 1, n * PAIR_ROWS)
        first = jnp.arange(SLICES + 1)[:, None, None] == 0
        hot_back = jnp.where(too_many, 0, num_hot)

        def go_out(i, acc):
            chip = jnp.where(i < hot_back, hot_at(i), none)
            hot_places = lax.dynamic_slice(places, (2 * jnp.minimum(chip, none - 1), PAIR_ROWS), (2, HOT_ROWS))
            hot_places = hot_places.reshape(2, SLICES, PAIR_ROWS).transpose(1, 0, 2)

            def to_root(root):
                return lambda *args: rows_out(n, root, *args, 4 + n + root)

            return lax.switch(chip, [to_root(k) for k in range(none + 1)], cold_src, spread(hot_places), jnp.where(first & (i > 0), -1, out_ids), acc)

        d_table = lax.fori_loop(0, jnp.maximum(hot_back, 1), go_out, jnp.zeros((rows_loc, width), jnp.float32))

        def extra_out(r, acc):
            back = swap(spread(window(place_pad, r * PAIR_ROWS, PAIR_ROWS)), 1, "rows_more")
            return add_rows(acc, window(ask_pad, r * PAIR_ROWS, PAIR_ROWS), back)

        d_table = lax.fori_loop(1, 1 + extra_rounds, extra_out, d_table)
        loss_note, d_table = lax.optimization_barrier((jnp.full((8, 128), loss_sum, jnp.float32), d_table))
        dw_one, dwi_one, dwi_two, loss_note = sum_over_devices(n, (dw_one, dwi_one, dwi_two), loss_note, 2)
        loss = loss_note[0, 0] / tok_total
        return loss, d_table, dw_one, dw_two, dwi_one, dwi_two

    return jax.shard_map(local_step, mesh=mesh, in_specs=(P("dp", None), P(), P(), P(), P(), P("dp", None), P(), P(), P("dp")), out_specs=(P(), P("dp", None), P(), P(), P(), P()), check_vma=False)
```
